512 devices in a mesh: mem: 2 (over y_hi), lat: 16 (over z), lon: 16 (over x, y_lo, core).
Axes of the slice: x: 4, y: 4 (y_hi: 2, y_lo: 2; y = y_hi * 2 + y_lo), z: 16, core: 2. Of those that a mesh axis runs over, the one named last changes fastest.
Arguments:
- control: bfloat16 [62, 3, 16, 16, 4608], P('mem', None, 'lat', 'lon'), may hold values from -6 to 6
- perturbs: bfloat16 [62, 3, 16, 16, 4608], P('mem', None, 'lat', 'lon'), may hold values from -0.75 to 0.75
- static_input: bfloat16 [3, 16, 16, 4608], P(None, 'lat', 'lon'), may hold values from -6 to 6
- lat_basis: bfloat16 [768, 384], replicated, may hold values from -0.21875 to 0.21875
- local_spectrum: float32 [384, 768], P(None, 'lat'), may hold values from 0.1 to 1
- static_spectrum: float32 [384, 768], P(None, 'lat'), may hold values from 0.1 to 1
- static_weight: float32 [3], replicated, may hold values from 0.2 to 0.8
Outputs:
- increment: float32 [3, 16, 16, 4608], P(None, 'lat', 'lon')
The draws below stay inside these ranges and needn't reach their ends.
All inputs are finite; a program needn't handle non-finite values.
Results may differ from the reference program's by a relative error of at most 0.0073.
Values may be sent and summed in bfloat16 or wider, within the bound.
A program may use at most 128 MiB of HBM per device.

```python
import math
import jax
import jax.numpy as jnp
from jax import lax

NLON = 1536
NLAT = 768
KLON = 768
KLAT = 384
LEV = 3
MEMBERS = 62
CELLS = 4608
N_LAT = 16
N_LON = 16


def block_levels(own_key, shape, cuts, low, high):
    factor_of, own = 1.0, jax.random.fold_in(own_key, 6)
    for axis_at, parts in cuts:
        heights = jnp.exp(jax.random.uniform(jax.random.fold_in(own, axis_at), (parts,), jnp.float32, low / len(cuts), high / len(cuts)))
        factor_of = factor_of * jnp.repeat(heights, shape[axis_at] // parts).reshape([-1 if axis == axis_at else 1 for axis in range(len(shape))])
    return factor_of


def gaussian(own_key, dims, scale, limit, shards=(), held_as=jnp.bfloat16):
    result = jax.random.normal(own_key, dims, jnp.float32) * scale
    if len(shards) > 0:
        result = block_levels(own_key, dims, shards, -0.22, 0.18) * result
    return jnp.clip(result, min=-limit, max=limit).astype(held_as)


def setup_inputs(seed: int = 0) -> dict:
    arg_keys = jax.random.split(jax.random.key(seed), 8)
    control = gaussian(arg_keys[0], (MEMBERS, LEV, N_LAT, N_LON, CELLS), 1.0, 6.0, ((0, 2), (2, 16), (3, 16)))
    perturbs = gaussian(arg_keys[1], (MEMBERS, LEV, N_LAT, N_LON, CELLS), 0.125, 0.75, ((0, 2), (2, 16), (3, 16)))
    static_input = gaussian(arg_keys[2], (LEV, N_LAT, N_LON, CELLS), 1.0, 6.0, ((1, 16), (2, 16)))
    lat_basis = gaussian(arg_keys[3], (NLAT, KLAT), NLAT ** -0.5, 0.21875)
    local_spectrum = jnp.clip(jnp.exp(math.log(1.0) - 2.3025851 * jax.random.uniform(arg_keys[4], (KLAT, KLON), jnp.float32) ** block_levels(arg_keys[4], (KLAT, KLON), ((1, 16),), -0.2, 0.2)), 0.1, 1.0)
    static_spectrum = jnp.clip(jnp.exp(math.log(1.0) - 2.3025851 * jax.random.uniform(arg_keys[5], (KLAT, KLON), jnp.float32) ** block_levels(arg_keys[5], (KLAT, KLON), ((1, 16),), -0.2, 0.2)), 0.1, 1.0)
    static_weight = jnp.clip(jax.random.uniform(arg_keys[6], (LEV,), jnp.float32, 0.2, 0.8), 0.2, 0.8)
    return dict(control=control, perturbs=perturbs, static_input=static_input, lat_basis=lat_basis, local_spectrum=local_spectrum, static_spectrum=static_spectrum, static_weight=static_weight)


def zonal_table():
    half = KLON // 2
    points = jnp.arange(NLON, dtype=jnp.int32)
    column = jnp.arange(KLON, dtype=jnp.int32)
    wave = jnp.where(column < half, column, column - half + 1)
    phase = points[:, None] * wave[None, :] % NLON
    angle = 2.0 * jnp.pi / NLON * phase.astype(jnp.float32)
    scale = jnp.sqrt(jnp.float32(2.0 / NLON))
    values = jnp.where(column[None, :] < half, jnp.cos(angle), jnp.sin(angle)) * scale
    return values.astype(jnp.bfloat16)

def to_plain(blocks):
    lead = blocks.shape[:-3]
    count = len(lead)
    lat_rows = NLAT // N_LAT
    lon_cols = NLON // N_LON
    shaped = blocks.reshape(lead + (N_LAT, N_LON, lat_rows, lon_cols))
    shaped = jnp.moveaxis(shaped, count + 2, count + 1)
    return shaped.reshape(lead + (NLAT, NLON))

def to_blocks(plain):
    lead = plain.shape[:-2]
    count = len(lead)
    lat_rows = NLAT // N_LAT
    lon_cols = NLON // N_LON
    shaped = plain.reshape(lead + (N_LAT, lat_rows, N_LON, lon_cols))
    shaped = jnp.moveaxis(shaped, count + 1, count + 2)
    return shaped.reshape(lead + (N_LAT, N_LON, lat_rows * lon_cols))

def filter_fields(fields, spectrum, zonal, merid):
    zonal_f = zonal.astype(jnp.float32)
    merid_f = merid.astype(jnp.float32)
    waves = jnp.einsum('lyn,nk->lyk', fields.astype(jnp.float32), zonal_f).astype(jnp.bfloat16)
    coef = jnp.einsum('lyk,yj->ljk', waves.astype(jnp.float32), merid_f) * spectrum[None]
    scaled = coef.astype(jnp.bfloat16)
    back = jnp.einsum('ljk,yj->lyk', scaled.astype(jnp.float32), merid_f).astype(jnp.bfloat16)
    grid = jnp.einsum('lyk,nk->lyn', back.astype(jnp.float32), zonal_f).astype(jnp.bfloat16)
    return grid

def reference(control, perturbs, static_input, lat_basis, local_spectrum, static_spectrum, static_weight):
    zonal = zonal_table()

    def add_member(total, pair):
        alpha, pert = pair
        grid = filter_fields(to_plain(alpha), local_spectrum, zonal, lat_basis)
        return (total + to_plain(pert).astype(jnp.float32) * grid.astype(jnp.float32), None)
    start = jnp.zeros((LEV, NLAT, NLON), jnp.float32)
    ensemble, unused = lax.scan(add_member, start, (control, perturbs))
    static_part = filter_fields(to_plain(static_input), static_spectrum, zonal, lat_basis).astype(jnp.float32)
    weight = static_weight[:, None, None]
    return to_blocks(weight * static_part + (1.0 - weight) * ensemble)
```

```python
import jax
import jax.numpy as jnp
import numpy as np
from jax import lax
from jax.experimental import pallas as pl
from jax.experimental.pallas import tpu as pltpu
from jax.sharding import PartitionSpec as P

NLON = 1536
KLON = 768
KLAT = 384
LEV = 3
ROWS = 48
COLS = 96
SUB = 3
PART = 16
CHUNKS = LEV * SUB
ACTIVE = 12
MESH = pl.DeviceIdType.MESH
F32 = jnp.float32
BF16 = jnp.bfloat16


def zonal_table():
    half = KLON // 2
    points = np.arange(NLON, dtype=np.int64)
    column = np.arange(KLON, dtype=np.int64)
    wave = np.where(column < half, column, column - half + 1)
    phase = points[:, None] * wave[None, :] % NLON
    angle = (np.float32(2.0 * np.pi / NLON) * phase.astype(np.float32)).astype(np.float32)
    scale = np.sqrt(np.float32(2.0 / NLON))
    values = np.where(column[None, :] < half, np.cos(angle), np.sin(angle)) * scale
    return values.astype(np.float32).astype(jnp.bfloat16)


def spread(tiles, lane):
    a, b, c = tiles
    rows = (
        a,
        pltpu.roll(jnp.where(lane >= 96, a, b), 32, 1),
        pltpu.roll(jnp.where(lane >= 64, b, c), 64, 1),
        pltpu.roll(c, 96, 1),
    )
    return [jnp.where(lane < COLS, r, 0.0) for r in rows]


def rows_of_members(src, level, dst, base):
    for g in range(4):
        n = 8 if g < 3 else 7
        lane = lax.broadcasted_iota(jnp.int32, (n, 128), 1)
        for q in range(12):
            v = src[level, g * 8 : g * 8 + n, q * 384 : (q + 1) * 384].astype(F32)
            for r, row in enumerate(spread((v[:, :128], v[:, 128:256], v[:, 256:]), lane)):
                dst[pl.ds(base + g * 8 * ROWS + 4 * q + r, n, stride=ROWS), :] = row


def kernel(
    weight_ref, control_hbm, perturbs_hbm, static_ref, lat_hbm, local_ref, stat_ref, zonal_hbm,
    out_ref,
    control, perturbs, lat, zonal, tmp, tmps, pert,
    a_send, a_recv, c_send, c_recv, e_send, e_recv, g_send, g_recv, m_send, m_recv, spc, spt, spec,
    in_sem, zon_sem, sa, ra, sc, rc, se, re, sg, rg, si, ri, sp,
):
    m = lax.axis_index("mem")
    z = lax.axis_index("lat")
    c = lax.axis_index("lon")
    quarter = lax.rem(z, 4)
    active = quarter < 3
    own_block = 3 * (z // 4) + quarter

    def far_first(i):
        step = (i + 1) // 2
        return 8 + jnp.where(lax.rem(i, 2) == 0, step, -step)

    loads = [
        pltpu.make_async_copy(control_hbm.at[k], control.at[k], in_sem.at[k]) for k in range(LEV)
    ]
    loads += [pltpu.make_async_copy(perturbs_hbm, perturbs, in_sem.at[3])]
    loads += [pltpu.make_async_copy(lat_hbm, lat, in_sem.at[4])]
    for copy in loads[:1]:
        copy.start()

    barrier = pltpu.get_barrier_semaphore()

    def greet(i, carry):
        pl.semaphore_signal(
            barrier, 1, device_id=(m, lax.rem(z + i, 16), c), device_id_type=MESH
        )
        pl.semaphore_signal(
            barrier, 1, device_id=(m, z, lax.rem(c + i, 16)), device_id_type=MESH
        )
        return carry

    lax.fori_loop(1, 16, greet, 0)
    pl.semaphore_signal(barrier, 1, device_id=(1 - m, z, c), device_id_type=MESH)

    for copy in loads[1:]:
        copy.start()
    zonal_loads = [
        pltpu.make_async_copy(
            zonal_hbm.at[pl.ds(b * COLS, COLS)], zonal.at[b, pl.ds(0, COLS)], zon_sem.at[b]
        )
        for b in range(16)
    ]
    for copy in zonal_loads:
        copy.start()

    lane3 = lax.broadcasted_iota(jnp.int32, (LEV, 128), 1)
    for q in range(12):
        v = static_ref[:, q * 384 : (q + 1) * 384].astype(F32)
        for r, row in enumerate(spread((v[:, :128], v[:, 128:256], v[:, 256:]), lane3)):
            tmps[pl.ds(4 * q + r, LEV, stride=ROWS), :] = row

    def prepare(level):
        rows_of_members(control, level, tmp, 0)
        tmp[pl.ds(31 * ROWS, ROWS), :] = tmps[pl.ds(pl.multiple_of(level * ROWS, 8), ROWS), :]

        def pack(peer, carry):
            for i in range(2):
                for s in range(SUB):
                    start = pl.multiple_of((2 * peer + i) * ROWS + s * PART, 8)
                    a_send[level * SUB + s, peer, i] = tmp[pl.ds(start, PART), :].astype(BF16)
            return carry

        lax.fori_loop(0, 16, pack, 0)

    def send_rows(level):
        for s in range(SUB):
            k = level * SUB + s
            a_recv[k, c] = a_send[k, c]

            def step(i, carry):
                to = lax.rem(c + i, 16)
                pltpu.make_async_remote_copy(
                    a_send.at[k, to], a_recv.at[k, c], sa.at[k], ra.at[k],
                    device_id=(m, z, to), device_id_type=MESH,
                ).start()
                return carry

            lax.fori_loop(1, 16, step, 0)

    loads[0].wait()
    prepare(0)
    spc[0] = local_ref[...]
    spc[1] = jnp.where(c == 15, stat_ref[...], local_ref[...])
    pl.semaphore_wait(barrier, 31)
    send_rows(0)

    def share(rows, at):
        return pltpu.make_async_remote_copy(
            spc.at[:, pl.ds(0, rows)], spt.at[:, pl.ds(at, rows)], sp.at[0], sp.at[1],
            device_id=(m, lax.rem(z + 15, 16), c), device_id_type=MESH,
        )

    for i, rows, at in ((1, 16, 48), (2, 32, 32), (3, 48, 16)):

        @pl.when(quarter == i)
        def _():
            share(rows, at).start()

    for i, rows in ((0, 48), (1, 32), (2, 16)):

        @pl.when(quarter == i)
        def _():
            spt[:, :rows, :] = spc[:, 48 - rows :, :]

    for k in (1, 2):
        loads[k].wait()

    def more(level, carry):
        prepare(level)
        send_rows(level)
        return carry

    lax.fori_loop(1, LEV, more, 0)

    for b in range(16):
        zonal[b, COLS:, :] = jnp.zeros((128 - COLS, KLON), BF16)
    for copy in zonal_loads:
        copy.wait()

    lane16 = lax.broadcasted_iota(jnp.int32, (PART, 128), 1)

    def to_waves(k, carry):
        pltpu.make_async_copy(
            a_recv.at[k, pl.ds(0, 15)], a_recv.at[k, pl.ds(0, 15)], ra.at[k]
        ).wait()
        strips = jnp.concatenate(
            [a_recv[k, b].reshape(2 * PART, 128) for b in range(16)], axis=1
        )
        table = zonal[...].reshape(16 * 128, KLON)
        waves = jnp.dot(strips, table, preferred_element_type=F32)
        for t in range(6):
            first = waves[:PART, t * 128 : (t + 1) * 128]
            second = waves[PART:, t * 128 : (t + 1) * 128]
            c_send[k, 2 * t] = jnp.where(lane16 < 64, first, pltpu.roll(second, 64, 1)).astype(BF16)
            c_send[k, 2 * t + 1] = jnp.where(
                lane16 < 64, pltpu.roll(first, 64, 1), second
            ).astype(BF16)
        level, s = k // SUB, lax.rem(k, SUB)

        @pl.when(active)
        def _():
            c_recv[level, z, s] = c_send[k, own_block]

        def step(i, inner):
            to = lax.rem(z + far_first(i), 16)
            part = lax.rem(to, 4)

            @pl.when(part < 3)
            def _():
                pltpu.make_async_remote_copy(
                    c_send.at[k, 3 * (to // 4) + part], c_recv.at[level, z, s], sc.at[k],
                    rc.at[level], device_id=(m, to, c), device_id_type=MESH,
                ).start()

            return inner

        lax.fori_loop(0, 15, step, 0)
        return carry

    lax.fori_loop(0, CHUNKS, to_waves, 0)

    loads[3].wait()
    loads[4].wait()

    def lay_out(level, carry):
        rows_of_members(perturbs, level, pert, level * (31 * ROWS))
        return carry

    lax.fori_loop(0, LEV, lay_out, 0)

    for i, rows, at in ((0, 16, 48), (1, 32, 32), (2, 48, 16)):

        @pl.when(quarter == i)
        def _():
            share(rows, at).wait_recv()

    @pl.when(active)
    def _():
        spec[...] = spt[...].reshape(128, KLAT).T

        def spectral(level, carry):
            pltpu.make_async_copy(
                c_recv.at[level, pl.ds(0, 15)], c_recv.at[level, pl.ds(0, 15)], rc.at[level]
            ).wait()
            merid = c_recv[level].reshape(16 * ROWS, 128)
            coef = lax.dot_general(
                lat[...], merid, (((0,), (0,)), ((), ())), preferred_element_type=F32
            )
            scaled = (coef * spec[...]).astype(BF16)
            for b in range(4):
                back = jnp.dot(
                    lat[pl.ds(b * 4 * ROWS, 4 * ROWS), :], scaled, preferred_element_type=F32
                )
                e_send[level, pl.ds(4 * b, 4)] = back.astype(BF16).reshape(4, SUB, PART, 128)

            for s in range(SUB):
                k = level * SUB + s
                e_recv[k, own_block] = e_send[level, z, s]

                def step(i, inner):
                    to = lax.rem(z + far_first(i), 16)
                    pltpu.make_async_remote_copy(
                        e_send.at[level, to, s], e_recv.at[k, own_block], se.at[k], re.at[k],
                        device_id=(m, to, c), device_id_type=MESH,
                    ).start()
                    return inner

                lax.fori_loop(0, 15, step, 0)
            return carry

        lax.fori_loop(0, LEV, spectral, 0)

    def to_grid(k, carry):
        for here, count in ((True, ACTIVE - 1), (False, ACTIVE)):

            @pl.when(active == here)
            def _():
                pltpu.make_async_copy(
                    e_recv.at[k, pl.ds(0, count)], e_recv.at[k, pl.ds(0, count)], re.at[k]
                ).wait()

        firsts, seconds = [], []
        for t in range(6):
            even = e_recv[k, 2 * t].astype(F32)
            odd = e_recv[k, 2 * t + 1].astype(F32)
            firsts.append(jnp.where(lane16 < 64, even, pltpu.roll(odd, 64, 1)))
            seconds.append(jnp.where(lane16 < 64, pltpu.roll(even, 64, 1), odd))
        rows = jnp.concatenate(
            [jnp.concatenate(firsts, axis=1), jnp.concatenate(seconds, axis=1)], axis=0
        ).astype(BF16)
        for b in range(4):
            grid = lax.dot_general(
                rows, zonal[pl.ds(4 * b, 4)].reshape(4 * 128, KLON), (((1,), (1,)), ((), ())),
                preferred_element_type=F32,
            ).astype(BF16)
            for i in range(4):
                g_send[k, 4 * b + i] = grid[:, i * 128 : (i + 1) * 128].reshape(2, PART, 128)
        g_recv[k, c] = g_send[k, c]

        def step(i, inner):
            to = lax.rem(c + i, 16)
            pltpu.make_async_remote_copy(
                g_send.at[k, to], g_recv.at[k, c], sg.at[k], rg.at[k],
                device_id=(m, z, to), device_id_type=MESH,
            ).start()
            return inner

        lax.fori_loop(1, 16, step, 0)
        return carry

    lax.fori_loop(0, CHUNKS, to_grid, 0)

    first_mem = jnp.where(m == 0, 1.0, 0.0).astype(F32)

    def across(k):
        return pltpu.make_async_remote_copy(
            m_send.at[k], m_recv.at[k], si.at[k], ri.at[k],
            device_id=(1 - m, z, c), device_id_type=MESH,
        )

    def product(k, carry):
        pltpu.make_async_copy(
            g_recv.at[k, pl.ds(0, 15)], g_recv.at[k, pl.ds(0, 15)], rg.at[k]
        ).wait()
        level, s = k // SUB, lax.rem(k, SUB)
        total = jnp.zeros((PART, 128), F32)
        for member in range(31):
            start = pl.multiple_of(level * (31 * ROWS) + member * ROWS + s * PART, 8)
            total += pert[pl.ds(start, PART), :] * g_recv[k, member // 2, member % 2].astype(F32)
        weight = weight_ref[level]
        static_part = g_recv[k, 15, 1].astype(F32)
        m_send[k] = first_mem * weight * static_part + (1.0 - weight) * total
        across(k).start()
        return carry

    lax.fori_loop(0, CHUNKS, product, 0)

    def finish(k, carry):
        across(k).wait()
        out_ref[k] = m_send[k] + m_recv[k]
        return carry

    lax.fori_loop(0, CHUNKS, finish, 0)

    for i, rows, at in ((1, 16, 48), (2, 32, 32), (3, 48, 16)):

        @pl.when(quarter == i)
        def _():
            share(rows, at).wait_send()

    def drain(k, carry):
        for ref, sem in ((a_send, sa), (g_send, sg)):
            pltpu.make_async_copy(
                ref.at[k, pl.ds(0, 15)], ref.at[k, pl.ds(0, 15)], sem.at[k]
            ).wait()
        for here, count in ((True, ACTIVE - 1), (False, ACTIVE)):

            @pl.when(active == here)
            def _():
                pltpu.make_async_copy(
                    c_send.at[k, pl.ds(0, count)], c_send.at[k, pl.ds(0, count)], sc.at[k]
                ).wait()

        @pl.when(active)
        def _():
            pltpu.make_async_copy(
                e_send.at[k // SUB, pl.ds(0, 15), 0], e_send.at[k // SUB, pl.ds(0, 15), 0], se.at[k]
            ).wait()

        return carry

    lax.fori_loop(0, CHUNKS, drain, 0)


def shards(
    control, perturbs, static_input, lat_basis, local_spectrum, static_spectrum, static_weight
):
    by_level = lambda a: jnp.swapaxes(a.reshape(31, LEV, ROWS * COLS), 0, 1)
    vmem = pl.BlockSpec(memory_space=pltpu.VMEM)
    hbm = pl.BlockSpec(memory_space=pltpu.HBM)
    dma = pltpu.SemaphoreType.DMA
    out = pl.pallas_call(
        kernel,
        out_shape=jax.ShapeDtypeStruct((CHUNKS, PART, 128), F32),
        in_specs=[
            pl.BlockSpec(memory_space=pltpu.SMEM), hbm, hbm, vmem, hbm, vmem, vmem, hbm,
        ],
        out_specs=vmem,
        scratch_shapes=[
            pltpu.VMEM((LEV, 31, ROWS * COLS), BF16),
            pltpu.VMEM((LEV, 31, ROWS * COLS), BF16),
            pltpu.VMEM((16 * ROWS, KLAT), BF16),
            pltpu.VMEM((16, 128, KLON), BF16),
            pltpu.VMEM((32 * ROWS, 128), F32),
            pltpu.VMEM((LEV * ROWS, 128), F32),
            pltpu.VMEM((LEV * 31 * ROWS, 128), F32),
            pltpu.VMEM((CHUNKS, 16, 2, PART, 128), BF16),
            pltpu.VMEM((CHUNKS, 16, 2, PART, 128), BF16),
            pltpu.VMEM((CHUNKS, ACTIVE, PART, 128), BF16),
            pltpu.VMEM((LEV, 16, SUB, PART, 128), BF16),
            pltpu.VMEM((LEV, 16, SUB, PART, 128), BF16),
            pltpu.VMEM((CHUNKS, ACTIVE, PART, 128), BF16),
            pltpu.VMEM((CHUNKS, 16, 2, PART, 128), BF16),
            pltpu.VMEM((CHUNKS, 16, 2, PART, 128), BF16),
            pltpu.VMEM((CHUNKS, PART, 128), F32),
            pltpu.VMEM((CHUNKS, PART, 128), F32),
            pltpu.VMEM((2, ROWS, KLAT), F32),
            pltpu.VMEM((2, 64, KLAT), F32),
            pltpu.VMEM((KLAT, 128), F32),
            dma((5,)),
            dma((16,)),
        ]
        + [dma((CHUNKS,))] * 3
        + [dma((LEV,))]
        + [dma((CHUNKS,))] * 6
        + [dma((2,))],
        compiler_params=pltpu.CompilerParams(
            collective_id=0, has_side_effects=True, vmem_limit_bytes=60 * 1024 * 1024
        ),
    )(
        static_weight,
        by_level(control),
        by_level(perturbs),
        static_input.reshape(LEV, ROWS * COLS),
        lat_basis,
        local_spectrum.T,
        static_spectrum.T,
        jnp.asarray(zonal_table()),
    )
    return out.reshape(LEV, ROWS, 128)[:, :, :COLS].reshape(LEV, 1, 1, ROWS * COLS)


def solution(mesh):
    in_specs = (
        P("mem", None, "lat", "lon", None),
        P("mem", None, "lat", "lon", None),
        P(None, "lat", "lon", None),
        P(),
        P(None, "lat"),
        P(None, "lat"),
        P(),
    )
    return jax.shard_map(
        shards, mesh=mesh, in_specs=in_specs, out_specs=P(None, "lat", "lon", None), check_vma=False
    )
```

```python
import jax
import jax.numpy as jnp
import numpy as np
from jax import lax
from jax.experimental import pallas as pl
from jax.experimental.pallas import tpu as pltpu
from jax.sharding import PartitionSpec as P

NLON = 1536
KLON = 768
KLAT = 384
LEV = 3
ROWS = 48
COLS = 96
SUB = 3
PART = 16
CHUNKS = LEV * SUB
ACTIVE = 12
EARLY = 8
MESH = pl.DeviceIdType.MESH
F32 = jnp.float32
BF16 = jnp.bfloat16


def zonal_table():
    half = KLON // 2
    points = np.arange(NLON, dtype=np.int64)
    column = np.arange(KLON, dtype=np.int64)
    wave = np.where(column < half, column, column - half + 1)
    phase = points[:, None] * wave[None, :] % NLON
    angle = (np.float32(2.0 * np.pi / NLON) * phase.astype(np.float32)).astype(np.float32)
    scale = np.sqrt(np.float32(2.0 / NLON))
    values = np.where(column[None, :] < half, np.cos(angle), np.sin(angle)) * scale
    return values.astype(np.float32).astype(jnp.bfloat16)


def spread(tiles, lane):
    a, b, c = tiles
    rows = (
        a,
        pltpu.roll(jnp.where(lane >= 96, a, b), 32, 1),
        pltpu.roll(jnp.where(lane >= 64, b, c), 64, 1),
        pltpu.roll(c, 96, 1),
    )
    return [jnp.where(lane < COLS, r, 0.0) for r in rows]


def pack_rows(rows, lane):
    return [jnp.where(lane < COLS, rows[j], pltpu.roll(rows[3], 96 - 32 * j, 1)) for j in range(3)]


def unpack_rows(packed, lane):
    turned = [pltpu.roll(packed[j], 32 + 32 * j, 1) for j in range(3)]
    last = jnp.where(lane < 32, turned[0], jnp.where(lane < 64, turned[1], turned[2]))
    return [packed[0], packed[1], packed[2], last]


def rows_of_members(src, level, dst, base):
    for g in range(4):
        n = 8 if g < 3 else 7
        lane = lax.broadcasted_iota(jnp.int32, (n, 128), 1)
        for q in range(12):
            v = src[level, g * 8 : g * 8 + n, q * 384 : (q + 1) * 384].astype(F32)
            for r, row in enumerate(spread((v[:, :128], v[:, 128:256], v[:, 256:]), lane)):
                dst[pl.ds(base + g * 8 * ROWS + 4 * q + r, n, stride=ROWS), :] = row


def kernel(
    weight_ref, control_hbm, perturbs_hbm, static_ref, lat_hbm, local_ref, stat_ref, zonal_hbm,
    out_ref,
    control, perturbs, lat, zonal, tmp, tmps, pert,
    a_send, a_recv, c_send, c_recv, e_send, e_recv, g_send, g_recv, m_send, m_recv, rows_out, flat, turned, spc, spt, spec,
    in_sem, zon_sem, sa, ra, sc, rc, se, re, sg, rg, si, ri, sp,
):
    m = lax.axis_index("mem")
    z = lax.axis_index("lat")
    c = lax.axis_index("lon")
    quarter = lax.rem(z, 4)
    core = lax.rem(c, 2)
    idle = 3 - 2 * core
    active = quarter != idle

    def block_of(device):
        part = lax.rem(device, 4)
        return 3 * (device // 4) + part - jnp.where(part > idle, 1, 0)

    own_block = block_of(z)

    def lon_peer(i):
        along, across = i // 4, 3 - lax.rem(i, 4)
        ahead = jnp.where(along == 3, 0, jnp.where(along == 2, 3, 2 - along))
        return 4 * lax.rem(c // 4 + ahead, 4) + lax.rem(lax.rem(c, 4) + across, 4)

    def far_first(i):
        step = (i + 1) // 2
        return 8 + jnp.where(lax.rem(i, 2) == 0, step, -step)

    loads = [
        pltpu.make_async_copy(control_hbm.at[k], control.at[k], in_sem.at[k]) for k in range(LEV)
    ]
    loads += [pltpu.make_async_copy(perturbs_hbm, perturbs, in_sem.at[3])]
    loads += [pltpu.make_async_copy(lat_hbm, lat, in_sem.at[4])]
    for copy in loads[:1]:
        copy.start()

    barrier = pltpu.get_barrier_semaphore()

    def greet(i, carry):
        pl.semaphore_signal(
            barrier, 1, device_id=(m, z, lax.rem(c + i, 16)), device_id_type=MESH
        )
        return carry

    def greet_far(i, carry):
        pl.semaphore_signal(
            barrier, 1, device_id=(m, lax.rem(z + far_first(i), 16), c), device_id_type=MESH
        )
        return carry

    lax.fori_loop(1, 16, greet, 0)
    lax.fori_loop(0, 15, greet_far, 0)
    pl.semaphore_signal(barrier, 1, device_id=(1 - m, z, c), device_id_type=MESH)

    for copy in loads[1:]:
        copy.start()
    zonal_loads = [
        pltpu.make_async_copy(
            zonal_hbm.at[pl.ds(b * COLS, COLS)], zonal.at[b, pl.ds(0, COLS)], zon_sem.at[b]
        )
        for b in range(16)
    ]
    for copy in zonal_loads:
        copy.start()

    lane3 = lax.broadcasted_iota(jnp.int32, (LEV, 128), 1)
    for q in range(12):
        v = static_ref[:, q * 384 : (q + 1) * 384].astype(F32)
        for r, row in enumerate(spread((v[:, :128], v[:, 128:256], v[:, 256:]), lane3)):
            tmps[pl.ds(4 * q + r, LEV, stride=ROWS), :] = row

    lane8 = lax.broadcasted_iota(jnp.int32, (8, 128), 1)

    def split(block):
        return [block[8 * j : 8 * j + 8, :] for j in range(3)]

    def prepare(level):
        rows_of_members(control, level, tmp, 0)
        tmp[pl.ds(31 * ROWS, ROWS), :] = tmps[pl.ds(pl.multiple_of(level * ROWS, 8), ROWS), :]

        def pack(peer, carry):
            for s in range(SUB):
                rows = []
                for i in range(2):
                    for h in range(2):
                        start = pl.multiple_of((2 * peer + i) * ROWS + s * PART + 8 * h, 8)
                        rows.append(tmp[pl.ds(start, 8), :])
                a_send[level * SUB + s, peer] = jnp.concatenate(
                    pack_rows(rows, lane8), axis=0
                ).astype(BF16)
            return carry

        lax.fori_loop(0, 16, pack, 0)

    def send_rows(k):
        a_recv[k, c] = a_send[k, c]

        def step(i, carry):
            to = lon_peer(i)
            pltpu.make_async_remote_copy(
                a_send.at[k, to], a_recv.at[k, c], sa.at[k], ra.at[k],
                device_id=(m, z, to), device_id_type=MESH,
            ).start()
            return carry

        lax.fori_loop(0, 15, step, 0)

    loads[0].wait()
    prepare(0)
    spc[0] = local_ref[...]
    spc[1] = jnp.where(c == 15, stat_ref[...], local_ref[...])
    pl.semaphore_wait(barrier, 31)
    for k in range(SUB):
        send_rows(k)

    def share(f, side, start, rows, at):
        return pltpu.make_async_remote_copy(
            spc.at[f, pl.ds(start, rows)], spt.at[f, pl.ds(at, rows)], sp.at[2 * f + (1 if side > 0 else 0)], sp.at[4 + f],
            device_id=(m, lax.rem(z + 16 + side, 16), c), device_id_type=MESH,
        )

    moves = (
        (0, 1, -1, 0, 16, 48), (0, 2, -1, 0, 32, 32), (0, 3, -1, 0, 48, 16),
        (1, 1, -1, 0, 16, 48), (1, 1, 1, 16, 32, 0), (1, 2, 1, 32, 16, 0),
    )
    stays = (
        (0, 0, 0, 48, 0), (0, 1, 16, 32, 0), (0, 2, 32, 16, 0),
        (1, 0, 0, 48, 0), (1, 2, 0, 32, 32), (1, 3, 0, 48, 16),
    )

    def for_shared(todo, receiving):
        for which, i, side, start, rows, at in moves:

            @pl.when((core == which) & (quarter == i + (side if receiving else 0)))
            def _():
                todo(share(0, side, start, rows, at))

                @pl.when(c == 15)
                def _():
                    todo(share(1, side, start, rows, at))

    for_shared(lambda copy: copy.start(), 0)

    for which, i, start, rows, at in stays:

        @pl.when((core == which) & (quarter == i))
        def _():
            spt[:, at : at + rows, :] = spc[:, start : start + rows, :]

    for k in (1, 2):
        loads[k].wait()

    for b in range(16):
        zonal[b, COLS:, :] = jnp.zeros((128 - COLS, KLON), BF16)
    for copy in zonal_loads:
        copy.wait()

    lane16 = lax.broadcasted_iota(jnp.int32, (PART, 128), 1)

    def lay_out(level, carry):
        rows_of_members(perturbs, level, pert, level * (31 * ROWS))
        return carry

    def ready_to_filter():
        loads[3].wait()
        loads[4].wait()
        for_shared(lambda copy: copy.wait_recv(), 1)

        @pl.when(active)
        def _():
            @pl.when(c < 15)
            def _():
                spt[1] = spt[0]

            spec[...] = spt[...].reshape(128, KLAT).T

    def filter_of(level):
        merid = c_recv[level].reshape(16 * ROWS, 128)
        coef = lax.dot_general(
            lat[...], merid, (((0,), (0,)), ((), ())), preferred_element_type=F32
        )
        scaled = (coef * spec[...]).astype(BF16)
        for b in range(4):
            back = jnp.dot(
                lat[pl.ds(b * 4 * ROWS, 4 * ROWS), :], scaled, preferred_element_type=F32
            )
            e_send[level, pl.ds(4 * b, 4)] = back.astype(BF16).reshape(4, SUB, PART, 128)

    def spectral(level, carry):
        pltpu.make_async_copy(
            c_recv.at[level, pl.ds(0, 15)], c_recv.at[level, pl.ds(0, 15)], rc.at[level]
        ).wait()
        filter_of(level)

        for s in range(SUB):
            k = level * SUB + s
            e_recv[k, own_block] = e_send[level, z, s]

            def step(i, inner):
                to = lax.rem(z + far_first(i), 16)
                pltpu.make_async_remote_copy(
                    e_send.at[level, to, s], e_recv.at[k, own_block], se.at[k], re.at[k],
                    device_id=(m, to, c), device_id_type=MESH,
                ).start()
                return inner

            lax.fori_loop(0, 15, step, 0)
        return carry

    def waves_of(k):
        strips = jnp.concatenate(
            [
                jnp.concatenate(
                    unpack_rows(split(a_recv[k, b].astype(F32)), lane8), axis=0
                ).astype(BF16)
                for b in range(16)
            ],
            axis=1,
        )
        table = zonal[...].reshape(16 * 128, KLON)
        waves = jnp.dot(strips, table, preferred_element_type=F32)
        for t in range(6):
            first = waves[:PART, t * 128 : (t + 1) * 128]
            second = waves[PART:, t * 128 : (t + 1) * 128]
            c_send[k, 2 * t] = jnp.where(lane16 < 64, first, pltpu.roll(second, 64, 1)).astype(BF16)
            c_send[k, 2 * t + 1] = jnp.where(
                lane16 < 64, pltpu.roll(first, 64, 1), second
            ).astype(BF16)

    def to_waves(k, carry):
        pltpu.make_async_copy(
            a_recv.at[k, pl.ds(0, 15)], a_recv.at[k, pl.ds(0, 15)], ra.at[k]
        ).wait()
        waves_of(k)
        level, s = k // SUB, lax.rem(k, SUB)

        @pl.when(active)
        def _():
            c_recv[level, z, s] = c_send[k, own_block]

        def step(i, inner):
            to = lax.rem(z + far_first(i), 16)

            @pl.when(lax.rem(to, 4) != idle)
            def _():
                pltpu.make_async_remote_copy(
                    c_send.at[k, block_of(to)], c_recv.at[level, z, s], sc.at[k],
                    rc.at[level], device_id=(m, to, c), device_id_type=MESH,
                ).start()

            return inner

        lax.fori_loop(0, 15, step, 0)

        @pl.when(k < CHUNKS - SUB)
        def _():
            @pl.when(s == 0)
            def _():
                prepare(level + 1)

            send_rows(k + SUB)

        @pl.when(k == 0)
        def _():
            ready_to_filter()

        @pl.when((k > 0) & (k <= LEV))
        def _():
            lay_out(k - 1, 0)

        @pl.when(active & (k == EARLY))
        def _():
            spectral(0, 0)

        return carry

    lax.fori_loop(0, CHUNKS, to_waves, 0)

    def turn(b, carry):
        turned[:, pl.ds(pl.multiple_of(b * 128, 128), 128)] = zonal[b].T
        return carry

    lax.fori_loop(0, 16, turn, 0)

    @pl.when(active)
    def _():
        lax.fori_loop(1, LEV, spectral, 0)

    def grid_of(k):
        firsts, seconds = [], []
        for t in range(6):
            even = e_recv[k, 2 * t].astype(F32)
            odd = e_recv[k, 2 * t + 1].astype(F32)
            firsts.append(jnp.where(lane16 < 64, even, pltpu.roll(odd, 64, 1)))
            seconds.append(jnp.where(lane16 < 64, pltpu.roll(even, 64, 1), odd))
        rows = jnp.concatenate(
            [jnp.concatenate(firsts, axis=1), jnp.concatenate(seconds, axis=1)], axis=0
        ).astype(BF16)
        for b in range(4):
            grid = lax.dot_general(
                rows, turned[:, b * 512 : (b + 1) * 512], (((1,), (0,)), ((), ())),
                preferred_element_type=F32,
            )
            for i in range(4):
                tiles = [
                    grid[8 * j : 8 * j + 8, i * 128 : (i + 1) * 128] for j in range(4)
                ]
                g_send[k, 4 * b + i] = jnp.concatenate(
                    pack_rows(tiles, lane8), axis=0
                ).astype(BF16)

    def to_grid(k, carry):
        for here, count in ((True, ACTIVE - 1), (False, ACTIVE)):

            @pl.when(active == here)
            def _():
                pltpu.make_async_copy(
                    e_recv.at[k, pl.ds(0, count)], e_recv.at[k, pl.ds(0, count)], re.at[k]
                ).wait()

        grid_of(k)
        g_recv[k, c] = g_send[k, c]

        def step(i, inner):
            to = lon_peer(i)
            pltpu.make_async_remote_copy(
                g_send.at[k, to], g_recv.at[k, c], sg.at[k], rg.at[k],
                device_id=(m, z, to), device_id_type=MESH,
            ).start()
            return inner

        lax.fori_loop(0, 15, step, 0)
        return carry

    lax.fori_loop(0, CHUNKS, to_grid, 0)

    first_mem = jnp.where(m == 0, 1.0, 0.0).astype(F32)

    def across(k):
        return pltpu.make_async_remote_copy(
            m_send.at[k], m_recv.at[k], si.at[k], ri.at[k],
            device_id=(1 - m, z, c), device_id_type=MESH,
        )

    def product_of(k, level, s):
        total = [jnp.zeros((8, 128), F32), jnp.zeros((8, 128), F32)]
        for peer in range(16):
            rows = unpack_rows(split(g_recv[k, peer].astype(F32)), lane8)
            for i in range(2 if peer < 15 else 1):
                for h in range(2):
                    start = level * (31 * ROWS) + (2 * peer + i) * ROWS + s * PART + 8 * h
                    total[h] += pert[pl.ds(pl.multiple_of(start, 8), 8), :] * rows[2 * i + h]
        weight = weight_ref[level]
        parts = [
            first_mem * weight * rows[2 + h] + (1.0 - weight) * total[h] for h in range(2)
        ]
        return jnp.concatenate(parts, axis=0)

    def product(k, carry):
        pltpu.make_async_copy(
            g_recv.at[k, pl.ds(0, 15)], g_recv.at[k, pl.ds(0, 15)], rg.at[k]
        ).wait()
        level, s = k // SUB, lax.rem(k, SUB)
        m_send[k] = product_of(k, level, s)
        across(k).start()
        return carry

    lax.fori_loop(0, CHUNKS, product, 0)

    def finish(k, carry):
        across(k).wait()
        rows_out[pl.ds(pl.multiple_of(k * PART, 8), PART), :] = m_send[k] + m_recv[k]
        return carry

    lax.fori_loop(0, CHUNKS, finish, 0)
    quads = LEV * ROWS // 4
    lane36 = lax.broadcasted_iota(jnp.int32, (quads, 128), 1)
    first, second, third, fourth = (rows_out[pl.ds(r, quads, stride=4), :] for r in range(4))
    second, third = pltpu.roll(second, 96, 1), pltpu.roll(third, 64, 1)
    fourth = pltpu.roll(fourth, 32, 1)
    flat[pl.ds(0, quads, stride=3), :] = jnp.where(lane36 < 96, first, second)
    flat[pl.ds(1, quads, stride=3), :] = jnp.where(lane36 < 64, second, third)
    flat[pl.ds(2, quads, stride=3), :] = jnp.where(lane36 < 32, third, fourth)

    out_ref[...] = flat[...].reshape(out_ref.shape)
    for_shared(lambda copy: copy.wait_send(), 0)

    def drain(k, carry):
        for ref, sem in ((a_send, sa), (g_send, sg)):
            pltpu.make_async_copy(
                ref.at[k, pl.ds(0, 15)], ref.at[k, pl.ds(0, 15)], sem.at[k]
            ).wait()
        for here, count in ((True, ACTIVE - 1), (False, ACTIVE)):

            @pl.when(active == here)
            def _():
                pltpu.make_async_copy(
                    c_send.at[k, pl.ds(0, count)], c_send.at[k, pl.ds(0, count)], sc.at[k]
                ).wait()

        @pl.when(active)
        def _():
            pltpu.make_async_copy(
                e_send.at[k // SUB, pl.ds(0, 15), 0], e_send.at[k // SUB, pl.ds(0, 15), 0], se.at[k]
            ).wait()

        return carry

    lax.fori_loop(0, CHUNKS, drain, 0)


def shards(
    control, perturbs, static_input, lat_basis, local_spectrum, static_spectrum, static_weight
):
    by_level = lambda a: jnp.swapaxes(a.reshape(31, LEV, ROWS * COLS), 0, 1)
    vmem = pl.BlockSpec(memory_space=pltpu.VMEM)
    hbm = pl.BlockSpec(memory_space=pltpu.HBM)
    dma = pltpu.SemaphoreType.DMA
    out = pl.pallas_call(
        kernel,
        out_shape=jax.ShapeDtypeStruct((LEV * ROWS * COLS // 128, 1, 128), F32),
        in_specs=[
            pl.BlockSpec(memory_space=pltpu.SMEM), hbm, hbm, vmem, hbm, vmem, vmem, hbm,
        ],
        out_specs=vmem,
        scratch_shapes=[
            pltpu.VMEM((LEV, 31, ROWS * COLS), BF16),
            pltpu.VMEM((LEV, 31, ROWS * COLS), BF16),
            pltpu.VMEM((16 * ROWS, KLAT), BF16),
            pltpu.VMEM((16, 128, KLON), BF16),
            pltpu.VMEM((32 * ROWS, 128), F32),
            pltpu.VMEM((LEV * ROWS, 128), F32),
            pltpu.VMEM((LEV * 31 * ROWS, 128), F32),
            pltpu.VMEM((CHUNKS, 16, 24, 128), BF16),
            pltpu.VMEM((CHUNKS, 16, 24, 128), BF16),
            pltpu.VMEM((CHUNKS, ACTIVE, PART, 128), BF16),
            pltpu.VMEM((LEV, 16, SUB, PART, 128), BF16),
            pltpu.VMEM((LEV, 16, SUB, PART, 128), BF16),
            pltpu.VMEM((CHUNKS, ACTIVE, PART, 128), BF16),
            pltpu.VMEM((CHUNKS, 16, 24, 128), BF16),
            pltpu.VMEM((CHUNKS, 16, 24, 128), BF16),
            pltpu.VMEM((CHUNKS, PART, 128), F32),
            pltpu.VMEM((CHUNKS, PART, 128), F32),
            pltpu.VMEM((LEV * ROWS, 128), F32),
            pltpu.VMEM((LEV * ROWS * COLS // 128, 128), F32),
            pltpu.VMEM((KLON, 16 * 128), BF16),
            pltpu.VMEM((2, ROWS, KLAT), F32),
            pltpu.VMEM((2, 64, KLAT), F32),
            pltpu.VMEM((KLAT, 128), F32),
            dma((5,)),
            dma((16,)),
        ]
        + [dma((CHUNKS,))] * 3
        + [dma((LEV,))]
        + [dma((CHUNKS,))] * 6
        + [dma((6,))],
        compiler_params=pltpu.CompilerParams(
            collective_id=0, has_side_effects=True, vmem_limit_bytes=60 * 1024 * 1024
        ),
    )(
        static_weight,
        by_level(control),
        by_level(perturbs),
        static_input.reshape(LEV, ROWS * COLS),
        lat_basis,
        local_spectrum.T,
        static_spectrum.T,
        jnp.asarray(zonal_table()),
    )
    return out.reshape(LEV, 1, 1, ROWS * COLS)


def solution(mesh):
    in_specs = (
        P("mem", None, "lat", "lon", None),
        P("mem", None, "lat", "lon", None),
        P(None, "lat", "lon", None),
        P(),
        P(None, "lat"),
        P(None, "lat"),
        P(),
    )
    return jax.shard_map(
        shards, mesh=mesh, in_specs=in_specs, out_specs=P(None, "lat", "lon", None), check_vma=False
    )
```

```python
import jax
import jax.numpy as jnp
import numpy as np
from jax import lax
from jax.experimental import pallas as pl
from jax.experimental.pallas import tpu as pltpu
from jax.sharding import PartitionSpec as P

NLON = 1536
KLON = 768
KLAT = 384
LEV = 3
ROWS = 48
COLS = 96
SUB = 3
PART = 16
CHUNKS = LEV * SUB
ACTIVE = 12
EARLY = 8
MESH = pl.DeviceIdType.MESH
F32 = jnp.float32
BF16 = jnp.bfloat16


def zonal_table():
    half = KLON // 2
    points = np.arange(NLON, dtype=np.int64)
    column = np.arange(KLON, dtype=np.int64)
    wave = np.where(column < half, column, column - half + 1)
    phase = points[:, None] * wave[None, :] % NLON
    angle = (np.float32(2.0 * np.pi / NLON) * phase.astype(np.float32)).astype(np.float32)
    scale = np.sqrt(np.float32(2.0 / NLON))
    values = np.where(column[None, :] < half, np.cos(angle), np.sin(angle)) * scale
    return values.astype(np.float32).astype(jnp.bfloat16)


def spread(tiles, lane):
    a, b, c = tiles
    rows = (
        a,
        pltpu.roll(jnp.where(lane >= 96, a, b), 32, 1),
        pltpu.roll(jnp.where(lane >= 64, b, c), 64, 1),
        pltpu.roll(c, 96, 1),
    )
    return [jnp.where(lane < COLS, r, 0.0) for r in rows]


def pack_rows(rows, lane):
    return [jnp.where(lane < COLS, rows[j], pltpu.roll(rows[3], 96 - 32 * j, 1)) for j in range(3)]


def unpack_rows(packed, lane):
    turned = [pltpu.roll(packed[j], 32 + 32 * j, 1) for j in range(3)]
    last = jnp.where(lane < 32, turned[0], jnp.where(lane < 64, turned[1], turned[2]))
    return [packed[0], packed[1], packed[2], last]


def rows_of_members(src, level, dst, base):
    for g in range(4):
        n = 8 if g < 3 else 7
        lane = lax.broadcasted_iota(jnp.int32, (n, 128), 1)
        for q in range(12):
            v = src[level, g * 8 : g * 8 + n, q * 384 : (q + 1) * 384].astype(F32)
            for r, row in enumerate(spread((v[:, :128], v[:, 128:256], v[:, 256:]), lane)):
                dst[pl.ds(base + g * 8 * ROWS + 4 * q + r, n, stride=ROWS), :] = row


def kernel(
    weight_hbm, control_hbm, perturbs_hbm, static_hbm, lat_hbm, local_hbm, stat_hbm, zonal_hbm,
    out_ref,
    weight_ref, static_ref, local_ref, stat_ref, control, perturbs, lat, zonal, tmp, tmps, pert,
    a_send, a_recv, c_send, c_recv, e_send, e_recv, g_send, g_recv, m_send, m_recv, rows_out, flat, turned, spc, spt, spec,
    in_sem, zon_sem, sa, ra, sc, rc, se, re, sg, rg, si, ri, sp,
):
    m = lax.axis_index("mem")
    z = lax.axis_index("lat")
    c = lax.axis_index("lon")
    quarter = lax.rem(z, 4)
    core = lax.rem(c, 2)
    idle = 3 - 2 * core
    active = quarter != idle

    def block_of(device):
        part = lax.rem(device, 4)
        return 3 * (device // 4) + part - jnp.where(part > idle, 1, 0)

    own_block = block_of(z)

    def lon_peer(i):
        along, across = i // 4, 3 - lax.rem(i, 4)
        ahead = jnp.where(along == 3, 0, jnp.where(along == 2, 3, 2 - along))
        return 4 * lax.rem(c // 4 + ahead, 4) + lax.rem(lax.rem(c, 4) + across, 4)

    def far_first(i):
        step = (i + 1) // 2
        return 8 + jnp.where(lax.rem(i, 2) == 0, step, -step)

    loads = [
        pltpu.make_async_copy(control_hbm.at[k], control.at[k], in_sem.at[k]) for k in range(LEV)
    ]
    loads += [pltpu.make_async_copy(perturbs_hbm, perturbs, in_sem.at[3])]
    loads += [pltpu.make_async_copy(lat_hbm, lat, in_sem.at[4])]
    barrier = pltpu.get_barrier_semaphore()

    def greet(i, carry):
        pl.semaphore_signal(
            barrier, 1, device_id=(m, z, lax.rem(c + i, 16)), device_id_type=MESH
        )
        return carry

    def greet_far(i, carry):
        pl.semaphore_signal(
            barrier, 1, device_id=(m, lax.rem(z + far_first(i), 16), c), device_id_type=MESH
        )
        return carry

    lax.fori_loop(0, 15, greet_far, 0)
    lax.fori_loop(1, 16, greet, 0)
    pl.semaphore_signal(barrier, 1, device_id=(1 - m, z, c), device_id_type=MESH)

    small = [
        pltpu.make_async_copy(source, target, in_sem.at[5 + i])
        for i, (source, target) in enumerate(
            (
                (static_hbm, static_ref), (local_hbm, local_ref), (stat_hbm, stat_ref),
                (weight_hbm, weight_ref),
            )
        )
    ]
    for copy in loads[:1] + small + loads[1:]:
        copy.start()
    zonal_loads = [
        pltpu.make_async_copy(
            zonal_hbm.at[pl.ds(b * COLS, COLS)], zonal.at[b, pl.ds(0, COLS)], zon_sem.at[b]
        )
        for b in range(16)
    ]
    for copy in zonal_loads:
        copy.start()

    for copy in small:
        copy.wait()
    lane3 = lax.broadcasted_iota(jnp.int32, (LEV, 128), 1)
    for q in range(12):
        v = static_ref[:, q * 384 : (q + 1) * 384].astype(F32)
        for r, row in enumerate(spread((v[:, :128], v[:, 128:256], v[:, 256:]), lane3)):
            tmps[pl.ds(4 * q + r, LEV, stride=ROWS), :] = row

    lane8 = lax.broadcasted_iota(jnp.int32, (8, 128), 1)

    def split(block):
        return [block[8 * j : 8 * j + 8, :] for j in range(3)]

    def prepare(level):
        rows_of_members(control, level, tmp, 0)
        tmp[pl.ds(31 * ROWS, ROWS), :] = tmps[pl.ds(pl.multiple_of(level * ROWS, 8), ROWS), :]

        def pack(peer, carry):
            for s in range(SUB):
                rows = []
                for i in range(2):
                    for h in range(2):
                        start = pl.multiple_of((2 * peer + i) * ROWS + s * PART + 8 * h, 8)
                        rows.append(tmp[pl.ds(start, 8), :])
                a_send[level * SUB + s, peer] = jnp.concatenate(
                    pack_rows(rows, lane8), axis=0
                ).astype(BF16)
            return carry

        lax.fori_loop(0, 16, pack, 0)

    def send_rows(k):
        a_recv[k, c] = a_send[k, c]

        def step(i, carry):
            to = lon_peer(i)
            pltpu.make_async_remote_copy(
                a_send.at[k, to], a_recv.at[k, c], sa.at[k], ra.at[k],
                device_id=(m, z, to), device_id_type=MESH,
            ).start()
            return carry

        lax.fori_loop(0, 15, step, 0)

    loads[0].wait()
    prepare(0)
    spc[0] = local_ref[...]
    spc[1] = jnp.where(c == 15, stat_ref[...], local_ref[...])
    pl.semaphore_wait(barrier, 31)
    for k in range(SUB):
        send_rows(k)

    def share(f, side, start, rows, at):
        return pltpu.make_async_remote_copy(
            spc.at[f, pl.ds(start, rows)], spt.at[f, pl.ds(at, rows)], sp.at[2 * f + (1 if side > 0 else 0)], sp.at[4 + f],
            device_id=(m, lax.rem(z + 16 + side, 16), c), device_id_type=MESH,
        )

    moves = (
        (0, 1, -1, 0, 16, 48), (0, 2, -1, 0, 32, 32), (0, 3, -1, 0, 48, 16),
        (1, 1, -1, 0, 16, 48), (1, 1, 1, 16, 32, 0), (1, 2, 1, 32, 16, 0),
    )
    stays = (
        (0, 0, 0, 48, 0), (0, 1, 16, 32, 0), (0, 2, 32, 16, 0),
        (1, 0, 0, 48, 0), (1, 2, 0, 32, 32), (1, 3, 0, 48, 16),
    )

    def for_shared(todo, receiving):
        for which, i, side, start, rows, at in moves:

            @pl.when((core == which) & (quarter == i + (side if receiving else 0)))
            def _():
                todo(share(0, side, start, rows, at))

                @pl.when(c == 15)
                def _():
                    todo(share(1, side, start, rows, at))

    for_shared(lambda copy: copy.start(), 0)

    for which, i, start, rows, at in stays:

        @pl.when((core == which) & (quarter == i))
        def _():
            spt[:, at : at + rows, :] = spc[:, start : start + rows, :]

    for k in (1, 2):
        loads[k].wait()

    for b in range(16):
        zonal[b, COLS:, :] = jnp.zeros((128 - COLS, KLON), BF16)
    for copy in zonal_loads:
        copy.wait()

    lane16 = lax.broadcasted_iota(jnp.int32, (PART, 128), 1)

    def lay_out(level, carry):
        rows_of_members(perturbs, level, pert, level * (31 * ROWS))
        return carry

    def ready_to_filter():
        loads[3].wait()
        loads[4].wait()
        for_shared(lambda copy: copy.wait_recv(), 1)

        @pl.when(active)
        def _():
            @pl.when(c < 15)
            def _():
                spt[1] = spt[0]

            spec[...] = spt[...].reshape(128, KLAT).T

    def filter_of(level):
        merid = c_recv[level].reshape(16 * ROWS, 128)
        coef = lax.dot_general(
            lat[...], merid, (((0,), (0,)), ((), ())), preferred_element_type=F32
        )
        scaled = (coef * spec[...]).astype(BF16)
        for b in range(4):
            back = jnp.dot(
                lat[pl.ds(b * 4 * ROWS, 4 * ROWS), :], scaled, preferred_element_type=F32
            )
            e_send[level, pl.ds(4 * b, 4)] = back.astype(BF16).reshape(4, SUB, PART, 128)

    def spectral(level, carry):
        pltpu.make_async_copy(
            c_recv.at[level, pl.ds(0, 15)], c_recv.at[level, pl.ds(0, 15)], rc.at[level]
        ).wait()
        filter_of(level)

        for s in range(SUB):
            k = level * SUB + s
            e_recv[k, own_block] = e_send[level, z, s]

            def step(i, inner):
                to = lax.rem(z + far_first(i), 16)
                pltpu.make_async_remote_copy(
                    e_send.at[level, to, s], e_recv.at[k, own_block], se.at[k], re.at[k],
                    device_id=(m, to, c), device_id_type=MESH,
                ).start()
                return inner

            lax.fori_loop(0, 15, step, 0)
        return carry

    def waves_of(k):
        strips = jnp.concatenate(
            [
                jnp.concatenate(
                    unpack_rows(split(a_recv[k, b].astype(F32)), lane8), axis=0
                ).astype(BF16)
                for b in range(16)
            ],
            axis=1,
        )
        table = zonal[...].reshape(16 * 128, KLON)
        waves = jnp.dot(strips, table, preferred_element_type=F32)
        for t in range(6):
            first = waves[:PART, t * 128 : (t + 1) * 128]
            second = waves[PART:, t * 128 : (t + 1) * 128]
            c_send[k, 2 * t] = jnp.where(lane16 < 64, first, pltpu.roll(second, 64, 1)).astype(BF16)
            c_send[k, 2 * t + 1] = jnp.where(
                lane16 < 64, pltpu.roll(first, 64, 1), second
            ).astype(BF16)

    def to_waves(k, carry):
        pltpu.make_async_copy(
            a_recv.at[k, pl.ds(0, 15)], a_recv.at[k, pl.ds(0, 15)], ra.at[k]
        ).wait()
        waves_of(k)
        level, s = k // SUB, lax.rem(k, SUB)

        @pl.when(active)
        def _():
            c_recv[level, z, s] = c_send[k, own_block]

        def step(i, inner):
            to = lax.rem(z + far_first(i), 16)

            @pl.when(lax.rem(to, 4) != idle)
            def _():
                pltpu.make_async_remote_copy(
                    c_send.at[k, block_of(to)], c_recv.at[level, z, s], sc.at[k],
                    rc.at[level], device_id=(m, to, c), device_id_type=MESH,
                ).start()

            return inner

        lax.fori_loop(0, 15, step, 0)

        @pl.when(k < CHUNKS - SUB)
        def _():
            @pl.when(s == 0)
            def _():
                prepare(level + 1)

            send_rows(k + SUB)

        @pl.when(k == 0)
        def _():
            ready_to_filter()

        @pl.when((k > 0) & (k <= LEV))
        def _():
            lay_out(k - 1, 0)

        @pl.when(active & (k == EARLY))
        def _():
            spectral(0, 0)

        return carry

    lax.fori_loop(0, CHUNKS, to_waves, 0)

    def turn(b, carry):
        turned[:, pl.ds(pl.multiple_of(b * 128, 128), 128)] = zonal[b].T
        return carry

    lax.fori_loop(0, 16, turn, 0)

    @pl.when(active)
    def _():
        lax.fori_loop(1, LEV, spectral, 0)

    def grid_of(k):
        firsts, seconds = [], []
        for t in range(6):
            even = e_recv[k, 2 * t].astype(F32)
            odd = e_recv[k, 2 * t + 1].astype(F32)
            firsts.append(jnp.where(lane16 < 64, even, pltpu.roll(odd, 64, 1)))
            seconds.append(jnp.where(lane16 < 64, pltpu.roll(even, 64, 1), odd))
        rows = jnp.concatenate(
            [jnp.concatenate(firsts, axis=1), jnp.concatenate(seconds, axis=1)], axis=0
        ).astype(BF16)
        for b in range(4):
            grid = lax.dot_general(
                rows, turned[:, b * 512 : (b + 1) * 512], (((1,), (0,)), ((), ())),
                preferred_element_type=F32,
            )
            for i in range(4):
                tiles = [
                    grid[8 * j : 8 * j + 8, i * 128 : (i + 1) * 128] for j in range(4)
                ]
                g_send[k, 4 * b + i] = jnp.concatenate(
                    pack_rows(tiles, lane8), axis=0
                ).astype(BF16)

    def to_grid(k, carry):
        for here, count in ((True, ACTIVE - 1), (False, ACTIVE)):

            @pl.when(active == here)
            def _():
                pltpu.make_async_copy(
                    e_recv.at[k, pl.ds(0, count)], e_recv.at[k, pl.ds(0, count)], re.at[k]
                ).wait()

        grid_of(k)
        g_recv[k, c] = g_send[k, c]

        def step(i, inner):
            to = lon_peer(i)
            pltpu.make_async_remote_copy(
                g_send.at[k, to], g_recv.at[k, c], sg.at[k], rg.at[k],
                device_id=(m, z, to), device_id_type=MESH,
            ).start()
            return inner

        lax.fori_loop(0, 15, step, 0)
        return carry

    lax.fori_loop(0, CHUNKS, to_grid, 0)

    first_mem = jnp.where(m == 0, 1.0, 0.0).astype(F32)

    def across(k):
        return pltpu.make_async_remote_copy(
            m_send.at[k], m_recv.at[k], si.at[k], ri.at[k],
            device_id=(1 - m, z, c), device_id_type=MESH,
        )

    def product_of(k, level, s):
        total = [jnp.zeros((8, 128), F32), jnp.zeros((8, 128), F32)]
        for peer in range(16):
            rows = unpack_rows(split(g_recv[k, peer].astype(F32)), lane8)
            for i in range(2 if peer < 15 else 1):
                for h in range(2):
                    start = level * (31 * ROWS) + (2 * peer + i) * ROWS + s * PART + 8 * h
                    total[h] += pert[pl.ds(pl.multiple_of(start, 8), 8), :] * rows[2 * i + h]
        weight = weight_ref[level]
        parts = [
            first_mem * weight * rows[2 + h] + (1.0 - weight) * total[h] for h in range(2)
        ]
        return jnp.concatenate(parts, axis=0)

    def product(k, carry):
        pltpu.make_async_copy(
            g_recv.at[k, pl.ds(0, 15)], g_recv.at[k, pl.ds(0, 15)], rg.at[k]
        ).wait()
        level, s = k // SUB, lax.rem(k, SUB)
        m_send[k] = product_of(k, level, s)
        across(k).start()
        return carry

    lax.fori_loop(0, CHUNKS, product, 0)

    def finish(k, carry):
        across(k).wait()
        rows_out[pl.ds(pl.multiple_of(k * PART, 8), PART), :] = m_send[k] + m_recv[k]
        return carry

    lax.fori_loop(0, CHUNKS, finish, 0)
    quads = LEV * ROWS // 4
    lane36 = lax.broadcasted_iota(jnp.int32, (quads, 128), 1)
    first, second, third, fourth = (rows_out[pl.ds(r, quads, stride=4), :] for r in range(4))
    second, third = pltpu.roll(second, 96, 1), pltpu.roll(third, 64, 1)
    fourth = pltpu.roll(fourth, 32, 1)
    flat[pl.ds(0, quads, stride=3), :] = jnp.where(lane36 < 96, first, second)
    flat[pl.ds(1, quads, stride=3), :] = jnp.where(lane36 < 64, second, third)
    flat[pl.ds(2, quads, stride=3), :] = jnp.where(lane36 < 32, third, fourth)

    out_ref[...] = flat[...].reshape(out_ref.shape)
    for_shared(lambda copy: copy.wait_send(), 0)

    def drain(k, carry):
        for ref, sem in ((a_send, sa), (g_send, sg)):
            pltpu.make_async_copy(
                ref.at[k, pl.ds(0, 15)], ref.at[k, pl.ds(0, 15)], sem.at[k]
            ).wait()
        for here, count in ((True, ACTIVE - 1), (False, ACTIVE)):

            @pl.when(active == here)
            def _():
                pltpu.make_async_copy(
                    c_send.at[k, pl.ds(0, count)], c_send.at[k, pl.ds(0, count)], sc.at[k]
                ).wait()

        @pl.when(active)
        def _():
            pltpu.make_async_copy(
                e_send.at[k // SUB, pl.ds(0, 15), 0], e_send.at[k // SUB, pl.ds(0, 15), 0], se.at[k]
            ).wait()

        return carry

    lax.fori_loop(0, CHUNKS, drain, 0)


def shards(
    control, perturbs, static_input, lat_basis, local_spectrum, static_spectrum, static_weight
):
    by_level = lambda a: jnp.swapaxes(a.reshape(31, LEV, ROWS * COLS), 0, 1)
    vmem = pl.BlockSpec(memory_space=pltpu.VMEM)
    hbm = pl.BlockSpec(memory_space=pltpu.HBM)
    dma = pltpu.SemaphoreType.DMA
    out = pl.pallas_call(
        kernel,
        out_shape=jax.ShapeDtypeStruct((LEV * ROWS * COLS // 128, 1, 128), F32),
        in_specs=[
            hbm, hbm, hbm, hbm, hbm, hbm, hbm, hbm,
        ],
        out_specs=vmem,
        scratch_shapes=[
            pltpu.SMEM((LEV,), F32),
            pltpu.VMEM((LEV, ROWS * COLS), BF16),
            pltpu.VMEM((ROWS, KLAT), F32),
            pltpu.VMEM((ROWS, KLAT), F32),
            pltpu.VMEM((LEV, 31, ROWS * COLS), BF16),
            pltpu.VMEM((LEV, 31, ROWS * COLS), BF16),
            pltpu.VMEM((16 * ROWS, KLAT), BF16),
            pltpu.VMEM((16, 128, KLON), BF16),
            pltpu.VMEM((32 * ROWS, 128), F32),
            pltpu.VMEM((LEV * ROWS, 128), F32),
            pltpu.VMEM((LEV * 31 * ROWS, 128), F32),
            pltpu.VMEM((CHUNKS, 16, 24, 128), BF16),
            pltpu.VMEM((CHUNKS, 16, 24, 128), BF16),
            pltpu.VMEM((CHUNKS, ACTIVE, PART, 128), BF16),
            pltpu.VMEM((LEV, 16, SUB, PART, 128), BF16),
            pltpu.VMEM((LEV, 16, SUB, PART, 128), BF16),
            pltpu.VMEM((CHUNKS, ACTIVE, PART, 128), BF16),
            pltpu.VMEM((CHUNKS, 16, 24, 128), BF16),
            pltpu.VMEM((CHUNKS, 16, 24, 128), BF16),
            pltpu.VMEM((CHUNKS, PART, 128), F32),
            pltpu.VMEM((CHUNKS, PART, 128), F32),
            pltpu.VMEM((LEV * ROWS, 128), F32),
            pltpu.VMEM((LEV * ROWS * COLS // 128, 128), F32),
            pltpu.VMEM((KLON, 16 * 128), BF16),
            pltpu.VMEM((2, ROWS, KLAT), F32),
            pltpu.VMEM((2, 64, KLAT), F32),
            pltpu.VMEM((KLAT, 128), F32),
            dma((9,)),
            dma((16,)),
        ]
        + [dma((CHUNKS,))] * 3
        + [dma((LEV,))]
        + [dma((CHUNKS,))] * 6
        + [dma((6,))],
        compiler_params=pltpu.CompilerParams(
            collective_id=0, has_side_effects=True, vmem_limit_bytes=60 * 1024 * 1024
        ),
    )(
        static_weight,
        by_level(control),
        by_level(perturbs),
        static_input.reshape(LEV, ROWS * COLS),
        lat_basis,
        local_spectrum.T,
        static_spectrum.T,
        jnp.asarray(zonal_table()),
    )
    return out.reshape(LEV, 1, 1, ROWS * COLS)


def solution(mesh):
    in_specs = (
        P("mem", None, "lat", "lon", None),
        P("mem", None, "lat", "lon", None),
        P(None, "lat", "lon", None),
        P(),
        P(None, "lat"),
        P(None, "lat"),
        P(),
    )
    return jax.shard_map(
        shards, mesh=mesh, in_specs=in_specs, out_specs=P(None, "lat", "lon", None), check_vma=False
    )
```

```python
import jax
import jax.numpy as jnp
import numpy as np
from jax import lax
from jax.experimental import pallas as pl
from jax.experimental.pallas import tpu as pltpu
from jax.sharding import PartitionSpec as P

NLON = 1536
KLON = 768
KLAT = 384
LEV = 3
ROWS = 48
COLS = 96
SUB = 3
PART = 16
CHUNKS = LEV * SUB
ACTIVE = 12
EARLY = 8
MESH = pl.DeviceIdType.MESH
F32 = jnp.float32
BF16 = jnp.bfloat16


def zonal_table():
    half = KLON // 2
    points = np.arange(NLON, dtype=np.int64)
    column = np.arange(KLON, dtype=np.int64)
    wave = np.where(column < half, column, column - half + 1)
    phase = points[:, None] * wave[None, :] % NLON
    angle = (np.float32(2.0 * np.pi / NLON) * phase.astype(np.float32)).astype(np.float32)
    scale = np.sqrt(np.float32(2.0 / NLON))
    values = np.where(column[None, :] < half, np.cos(angle), np.sin(angle)) * scale
    return values.astype(np.float32).astype(jnp.bfloat16)


def spread(tiles, lane):
    a, b, c = tiles
    rows = (
        a,
        pltpu.roll(jnp.where(lane >= 96, a, b), 32, 1),
        pltpu.roll(jnp.where(lane >= 64, b, c), 64, 1),
        pltpu.roll(c, 96, 1),
    )
    return [jnp.where(lane < COLS, r, 0.0) for r in rows]


def pack_rows(rows, lane):
    return [jnp.where(lane < COLS, rows[j], pltpu.roll(rows[3], 96 - 32 * j, 1)) for j in range(3)]


def unpack_rows(packed, lane):
    turned = [pltpu.roll(packed[j], 32 + 32 * j, 1) for j in range(3)]
    last = jnp.where(lane < 32, turned[0], jnp.where(lane < 64, turned[1], turned[2]))
    return [packed[0], packed[1], packed[2], last]


def rows_of_members(src, level, dst, base):
    for g in range(4):
        n = 8 if g < 3 else 7
        lane = lax.broadcasted_iota(jnp.int32, (n, 128), 1)
        for q in range(12):
            v = src[level, g * 8 : g * 8 + n, q * 384 : (q + 1) * 384].astype(F32)
            for r, row in enumerate(spread((v[:, :128], v[:, 128:256], v[:, 256:]), lane)):
                dst[pl.ds(base + g * 8 * ROWS + 4 * q + r, n, stride=ROWS), :] = row


def kernel(
    weight_hbm, control_hbm, perturbs_hbm, static_hbm, lat_hbm, local_hbm, stat_hbm, zonal_hbm,
    out_ref,
    weight_ref, static_ref, local_ref, stat_ref, control, perturbs, lat, zonal, tmp, tmps, pert,
    a_send, a_recv, c_send, c_recv, e_send, e_recv, g_send, g_recv, m_send, m_recv, rows_out, flat, turned, spc, spt, spec,
    in_sem, zon_sem, sa, ra, sc, rc, se, re, sg, rg, si, ri, sp,
):
    m = lax.axis_index("mem")
    z = lax.axis_index("lat")
    c = lax.axis_index("lon")
    quarter = lax.rem(z, 4)
    core = lax.rem(c, 2)

    def plan_of(level):
        return jnp.where(level == 1, 1, 0)

    def idle(level):
        return 3 - 2 * core - plan_of(level)

    def active(level):
        return quarter != idle(level)

    def block_of(device, level):
        part = lax.rem(device, 4)
        return 3 * (device // 4) + part - jnp.where(part > idle(level), 1, 0)


    def lon_peer(i):
        along, across = i // 4, 3 - lax.rem(i, 4)
        ahead = jnp.where(along == 3, 0, jnp.where(along == 2, 3, 2 - along))
        return 4 * lax.rem(c // 4 + ahead, 4) + lax.rem(lax.rem(c, 4) + across, 4)

    def far_first(i):
        step = (i + 1) // 2
        return 8 + jnp.where(lax.rem(i, 2) == 0, step, -step)

    loads = [
        pltpu.make_async_copy(control_hbm.at[k], control.at[k], in_sem.at[k]) for k in range(LEV)
    ]
    loads += [pltpu.make_async_copy(perturbs_hbm, perturbs, in_sem.at[3])]
    loads += [pltpu.make_async_copy(lat_hbm, lat, in_sem.at[4])]
    barrier = pltpu.get_barrier_semaphore()

    def greet(i, carry):
        pl.semaphore_signal(
            barrier, 1, device_id=(m, z, lax.rem(c + i, 16)), device_id_type=MESH
        )
        return carry

    def greet_far(i, carry):
        pl.semaphore_signal(
            barrier, 1, device_id=(m, lax.rem(z + far_first(i), 16), c), device_id_type=MESH
        )
        return carry

    lax.fori_loop(0, 15, greet_far, 0)
    lax.fori_loop(1, 16, greet, 0)
    pl.semaphore_signal(barrier, 1, device_id=(1 - m, z, c), device_id_type=MESH)

    small = [
        pltpu.make_async_copy(source, target, in_sem.at[5 + i])
        for i, (source, target) in enumerate(
            (
                (static_hbm, static_ref), (local_hbm, local_ref), (stat_hbm, stat_ref),
                (weight_hbm, weight_ref),
            )
        )
    ]
    for copy in loads[:1] + small + loads[1:]:
        copy.start()
    zonal_loads = [
        pltpu.make_async_copy(
            zonal_hbm.at[pl.ds(b * COLS, COLS)], zonal.at[b, pl.ds(0, COLS)], zon_sem.at[b]
        )
        for b in range(16)
    ]
    for copy in zonal_loads:
        copy.start()

    for copy in small:
        copy.wait()
    lane3 = lax.broadcasted_iota(jnp.int32, (LEV, 128), 1)
    for q in range(12):
        v = static_ref[:, q * 384 : (q + 1) * 384].astype(F32)
        for r, row in enumerate(spread((v[:, :128], v[:, 128:256], v[:, 256:]), lane3)):
            tmps[pl.ds(4 * q + r, LEV, stride=ROWS), :] = row

    lane8 = lax.broadcasted_iota(jnp.int32, (8, 128), 1)

    def split(block):
        return [block[8 * j : 8 * j + 8, :] for j in range(3)]

    def prepare(level):
        rows_of_members(control, level, tmp, 0)
        tmp[pl.ds(31 * ROWS, ROWS), :] = tmps[pl.ds(pl.multiple_of(level * ROWS, 8), ROWS), :]

        def pack(peer, carry):
            for s in range(SUB):
                rows = []
                for i in range(2):
                    for h in range(2):
                        start = pl.multiple_of((2 * peer + i) * ROWS + s * PART + 8 * h, 8)
                        rows.append(tmp[pl.ds(start, 8), :])
                a_send[level * SUB + s, peer] = jnp.concatenate(
                    pack_rows(rows, lane8), axis=0
                ).astype(BF16)
            return carry

        lax.fori_loop(0, 16, pack, 0)

    def send_rows(k):
        a_recv[k, c] = a_send[k, c]

        def step(i, carry):
            to = lon_peer(i)
            pltpu.make_async_remote_copy(
                a_send.at[k, to], a_recv.at[k, c], sa.at[k], ra.at[k],
                device_id=(m, z, to), device_id_type=MESH,
            ).start()
            return carry

        lax.fori_loop(0, 15, step, 0)

    loads[0].wait()
    prepare(0)
    spc[0] = local_ref[...]
    spc[1] = jnp.where(c == 15, stat_ref[...], local_ref[...])
    pl.semaphore_wait(barrier, 31)
    for k in range(SUB):
        send_rows(k)

    def share(plan, f, side, start, rows, at):
        send = 4 * plan + 2 * f + (1 if side > 0 else 0)
        return pltpu.make_async_remote_copy(
            spc.at[f, pl.ds(start, rows)], spt.at[plan, f, pl.ds(at, rows)],
            sp.at[send], sp.at[8 + 2 * plan + f],
            device_id=(m, lax.rem(z + 16 + side, 16), c), device_id_type=MESH,
        )

    pieces = []
    for plan in range(2):
        for which in range(2):
            users = [i for i in range(4) if i != 3 - 2 * which - plan]
            for block, user in enumerate(users):
                for owner in range(4):
                    low = max(64 * block, ROWS * owner)
                    high = min(64 * block + 64, ROWS * owner + ROWS)
                    if low < high:
                        start, at = low - ROWS * owner, low - 64 * block
                        pieces.append((plan, which, owner, user, start, high - low, at))

    def for_shared(todo, receiving):
        for plan, which, owner, user, start, rows, at in pieces:
            if owner == user:
                continue

            @pl.when((core == which) & (quarter == (user if receiving else owner)))
            def _():
                todo(share(plan, 0, user - owner, start, rows, at))

                @pl.when(c == 15)
                def _():
                    todo(share(plan, 1, user - owner, start, rows, at))

    for_shared(lambda copy: copy.start(), 0)

    for plan, which, owner, user, start, rows, at in pieces:
        if owner == user:

            @pl.when((core == which) & (quarter == owner))
            def _():
                spt[plan, :, at : at + rows, :] = spc[:, start : start + rows, :]

    for k in (1, 2):
        loads[k].wait()

    for b in range(16):
        zonal[b, COLS:, :] = jnp.zeros((128 - COLS, KLON), BF16)
    for copy in zonal_loads:
        copy.wait()

    lane16 = lax.broadcasted_iota(jnp.int32, (PART, 128), 1)

    def lay_out(level, carry):
        rows_of_members(perturbs, level, pert, level * (31 * ROWS))
        return carry

    def ready_to_filter():
        loads[3].wait()
        loads[4].wait()
        for_shared(lambda copy: copy.wait_recv(), 1)

        for plan in range(2):

            @pl.when(active(plan))
            def _():
                @pl.when(c < 15)
                def _():
                    spt[plan, 1] = spt[plan, 0]

                spec[plan] = spt[plan].reshape(128, KLAT).T

    def filter_of(level):
        merid = c_recv[level].reshape(16 * ROWS, 128)
        coef = lax.dot_general(
            lat[...], merid, (((0,), (0,)), ((), ())), preferred_element_type=F32
        )
        scaled = (coef * spec[plan_of(level)]).astype(BF16)
        for b in range(4):
            back = jnp.dot(
                lat[pl.ds(b * 4 * ROWS, 4 * ROWS), :], scaled, preferred_element_type=F32
            )
            e_send[level, pl.ds(4 * b, 4)] = back.astype(BF16).reshape(4, SUB, PART, 128)

    def spectral(level, carry):
        pltpu.make_async_copy(
            c_recv.at[level, pl.ds(0, 15)], c_recv.at[level, pl.ds(0, 15)], rc.at[level]
        ).wait()
        filter_of(level)
        own_block = block_of(z, level)

        for s in range(SUB):
            k = level * SUB + s
            e_recv[k, own_block] = e_send[level, z, s]

            def step(i, inner):
                to = lax.rem(z + far_first(i), 16)
                pltpu.make_async_remote_copy(
                    e_send.at[level, to, s], e_recv.at[k, own_block], se.at[k], re.at[k],
                    device_id=(m, to, c), device_id_type=MESH,
                ).start()
                return inner

            lax.fori_loop(0, 15, step, 0)
        return carry

    def waves_of(k):
        strips = jnp.concatenate(
            [
                jnp.concatenate(
                    unpack_rows(split(a_recv[k, b].astype(F32)), lane8), axis=0
                ).astype(BF16)
                for b in range(16)
            ],
            axis=1,
        )
        table = zonal[...].reshape(16 * 128, KLON)
        waves = jnp.dot(strips, table, preferred_element_type=F32)
        for t in range(6):
            first = waves[:PART, t * 128 : (t + 1) * 128]
            second = waves[PART:, t * 128 : (t + 1) * 128]
            c_send[k, 2 * t] = jnp.where(lane16 < 64, first, pltpu.roll(second, 64, 1)).astype(BF16)
            c_send[k, 2 * t + 1] = jnp.where(
                lane16 < 64, pltpu.roll(first, 64, 1), second
            ).astype(BF16)

    def to_waves(k, carry):
        pltpu.make_async_copy(
            a_recv.at[k, pl.ds(0, 15)], a_recv.at[k, pl.ds(0, 15)], ra.at[k]
        ).wait()
        waves_of(k)
        level, s = k // SUB, lax.rem(k, SUB)

        @pl.when(active(level))
        def _():
            c_recv[level, z, s] = c_send[k, block_of(z, level)]

        def step(i, inner):
            to = lax.rem(z + far_first(i), 16)

            @pl.when(lax.rem(to, 4) != idle(level))
            def _():
                pltpu.make_async_remote_copy(
                    c_send.at[k, block_of(to, level)], c_recv.at[level, z, s], sc.at[k],
                    rc.at[level], device_id=(m, to, c), device_id_type=MESH,
                ).start()

            return inner

        lax.fori_loop(0, 15, step, 0)

        @pl.when(k < CHUNKS - SUB)
        def _():
            @pl.when(s == 0)
            def _():
                prepare(level + 1)

            send_rows(k + SUB)

        @pl.when(k == CHUNKS - LEV - 2)
        def _():
            ready_to_filter()

        @pl.when((k >= CHUNKS - LEV - 1) & (k < CHUNKS - 1))
        def _():
            lay_out(k - (CHUNKS - LEV - 1), 0)

        @pl.when(active(0) & (k == EARLY))
        def _():
            spectral(0, 0)

        return carry

    lax.fori_loop(0, CHUNKS, to_waves, 0)

    def turn(b, carry):
        turned[:, pl.ds(pl.multiple_of(b * 128, 128), 128)] = zonal[b].T
        return carry

    lax.fori_loop(0, 16, turn, 0)

    for level in range(1, LEV):

        @pl.when(active(level))
        def _():
            spectral(level, 0)

    def grid_of(k):
        firsts, seconds = [], []
        for t in range(6):
            even = e_recv[k, 2 * t].astype(F32)
            odd = e_recv[k, 2 * t + 1].astype(F32)
            firsts.append(jnp.where(lane16 < 64, even, pltpu.roll(odd, 64, 1)))
            seconds.append(jnp.where(lane16 < 64, pltpu.roll(even, 64, 1), odd))
        rows = jnp.concatenate(
            [jnp.concatenate(firsts, axis=1), jnp.concatenate(seconds, axis=1)], axis=0
        ).astype(BF16)
        for b in range(4):
            grid = lax.dot_general(
                rows, turned[:, b * 512 : (b + 1) * 512], (((1,), (0,)), ((), ())),
                preferred_element_type=F32,
            )
            for i in range(4):
                tiles = [
                    grid[8 * j : 8 * j + 8, i * 128 : (i + 1) * 128] for j in range(4)
                ]
                g_send[k, 4 * b + i] = jnp.concatenate(
                    pack_rows(tiles, lane8), axis=0
                ).astype(BF16)

    def to_grid(k, carry):
        for here, count in ((True, ACTIVE - 1), (False, ACTIVE)):

            @pl.when(active(k // SUB) == here)
            def _():
                pltpu.make_async_copy(
                    e_recv.at[k, pl.ds(0, count)], e_recv.at[k, pl.ds(0, count)], re.at[k]
                ).wait()

        grid_of(k)
        g_recv[k, c] = g_send[k, c]

        def step(i, inner):
            to = lon_peer(i)
            pltpu.make_async_remote_copy(
                g_send.at[k, to], g_recv.at[k, c], sg.at[k], rg.at[k],
                device_id=(m, z, to), device_id_type=MESH,
            ).start()
            return inner

        lax.fori_loop(0, 15, step, 0)
        return carry

    lax.fori_loop(0, CHUNKS, to_grid, 0)

    first_mem = jnp.where(m == 0, 1.0, 0.0).astype(F32)

    def across(k):
        return pltpu.make_async_remote_copy(
            m_send.at[k], m_recv.at[k], si.at[k], ri.at[k],
            device_id=(1 - m, z, c), device_id_type=MESH,
        )

    def product_of(k, level, s):
        total = [jnp.zeros((8, 128), F32), jnp.zeros((8, 128), F32)]
        for peer in range(16):
            rows = unpack_rows(split(g_recv[k, peer].astype(F32)), lane8)
            for i in range(2 if peer < 15 else 1):
                for h in range(2):
                    start = level * (31 * ROWS) + (2 * peer + i) * ROWS + s * PART + 8 * h
                    total[h] += pert[pl.ds(pl.multiple_of(start, 8), 8), :] * rows[2 * i + h]
        weight = weight_ref[level]
        parts = [
            first_mem * weight * rows[2 + h] + (1.0 - weight) * total[h] for h in range(2)
        ]
        return jnp.concatenate(parts, axis=0)

    def product(k, carry):
        pltpu.make_async_copy(
            g_recv.at[k, pl.ds(0, 15)], g_recv.at[k, pl.ds(0, 15)], rg.at[k]
        ).wait()
        level, s = k // SUB, lax.rem(k, SUB)
        m_send[k] = product_of(k, level, s)
        across(k).start()
        return carry

    lax.fori_loop(0, CHUNKS, product, 0)

    def finish(k, carry):
        across(k).wait()
        rows_out[pl.ds(pl.multiple_of(k * PART, 8), PART), :] = m_send[k] + m_recv[k]
        return carry

    lax.fori_loop(0, CHUNKS, finish, 0)
    quads = LEV * ROWS // 4
    lane36 = lax.broadcasted_iota(jnp.int32, (quads, 128), 1)
    first, second, third, fourth = (rows_out[pl.ds(r, quads, stride=4), :] for r in range(4))
    second, third = pltpu.roll(second, 96, 1), pltpu.roll(third, 64, 1)
    fourth = pltpu.roll(fourth, 32, 1)
    flat[pl.ds(0, quads, stride=3), :] = jnp.where(lane36 < 96, first, second)
    flat[pl.ds(1, quads, stride=3), :] = jnp.where(lane36 < 64, second, third)
    flat[pl.ds(2, quads, stride=3), :] = jnp.where(lane36 < 32, third, fourth)

    out_ref[...] = flat[...].reshape(out_ref.shape)
    for_shared(lambda copy: copy.wait_send(), 0)

    def drain(k, carry):
        for ref, sem in ((a_send, sa), (g_send, sg)):
            pltpu.make_async_copy(
                ref.at[k, pl.ds(0, 15)], ref.at[k, pl.ds(0, 15)], sem.at[k]
            ).wait()
        for here, count in ((True, ACTIVE - 1), (False, ACTIVE)):

            @pl.when(active(k // SUB) == here)
            def _():
                pltpu.make_async_copy(
                    c_send.at[k, pl.ds(0, count)], c_send.at[k, pl.ds(0, count)], sc.at[k]
                ).wait()

        @pl.when(active(k // SUB))
        def _():
            pltpu.make_async_copy(
                e_send.at[k // SUB, pl.ds(0, 15), 0], e_send.at[k // SUB, pl.ds(0, 15), 0], se.at[k]
            ).wait()

        return carry

    lax.fori_loop(0, CHUNKS, drain, 0)


def shards(
    control, perturbs, static_input, lat_basis, local_spectrum, static_spectrum, static_weight
):
    by_level = lambda a: jnp.swapaxes(a.reshape(31, LEV, ROWS * COLS), 0, 1)
    vmem = pl.BlockSpec(memory_space=pltpu.VMEM)
    hbm = pl.BlockSpec(memory_space=pltpu.HBM)
    dma = pltpu.SemaphoreType.DMA
    out = pl.pallas_call(
        kernel,
        out_shape=jax.ShapeDtypeStruct((LEV * ROWS * COLS // 128, 1, 128), F32),
        in_specs=[
            hbm, hbm, hbm, hbm, hbm, hbm, hbm, hbm,
        ],
        out_specs=vmem,
        scratch_shapes=[
            pltpu.SMEM((LEV,), F32),
            pltpu.VMEM((LEV, ROWS * COLS), BF16),
            pltpu.VMEM((ROWS, KLAT), F32),
            pltpu.VMEM((ROWS, KLAT), F32),
            pltpu.VMEM((LEV, 31, ROWS * COLS), BF16),
            pltpu.VMEM((LEV, 31, ROWS * COLS), BF16),
            pltpu.VMEM((16 * ROWS, KLAT), BF16),
            pltpu.VMEM((16, 128, KLON), BF16),
            pltpu.VMEM((32 * ROWS, 128), F32),
            pltpu.VMEM((LEV * ROWS, 128), F32),
            pltpu.VMEM((LEV * 31 * ROWS, 128), F32),
            pltpu.VMEM((CHUNKS, 16, 24, 128), BF16),
            pltpu.VMEM((CHUNKS, 16, 24, 128), BF16),
            pltpu.VMEM((CHUNKS, ACTIVE, PART, 128), BF16),
            pltpu.VMEM((LEV, 16, SUB, PART, 128), BF16),
            pltpu.VMEM((LEV, 16, SUB, PART, 128), BF16),
            pltpu.VMEM((CHUNKS, ACTIVE, PART, 128), BF16),
            pltpu.VMEM((CHUNKS, 16, 24, 128), BF16),
            pltpu.VMEM((CHUNKS, 16, 24, 128), BF16),
            pltpu.VMEM((CHUNKS, PART, 128), F32),
            pltpu.VMEM((CHUNKS, PART, 128), F32),
            pltpu.VMEM((LEV * ROWS, 128), F32),
            pltpu.VMEM((LEV * ROWS * COLS // 128, 128), F32),
            pltpu.VMEM((KLON, 16 * 128), BF16),
            pltpu.VMEM((2, ROWS, KLAT), F32),
            pltpu.VMEM((2, 2, 64, KLAT), F32),
            pltpu.VMEM((2, KLAT, 128), F32),
            dma((9,)),
            dma((16,)),
        ]
        + [dma((CHUNKS,))] * 3
        + [dma((LEV,))]
        + [dma((CHUNKS,))] * 6
        + [dma((12,))],
        compiler_params=pltpu.CompilerParams(
            collective_id=0, has_side_effects=True, vmem_limit_bytes=60 * 1024 * 1024
        ),
    )(
        static_weight,
        by_level(control),
        by_level(perturbs),
        static_input.reshape(LEV, ROWS * COLS),
        lat_basis,
        local_spectrum.T,
        static_spectrum.T,
        jnp.asarray(zonal_table()),
    )
    return out.reshape(LEV, 1, 1, ROWS * COLS)


def solution(mesh):
    in_specs = (
        P("mem", None, "lat", "lon", None),
        P("mem", None, "lat", "lon", None),
        P(None, "lat", "lon", None),
        P(),
        P(None, "lat"),
        P(None, "lat"),
        P(),
    )
    return jax.shard_map(
        shards, mesh=mesh, in_specs=in_specs, out_specs=P(None, "lat", "lon", None), check_vma=False
    )
```

```python
import jax
import jax.numpy as jnp
import numpy as np
from jax import lax
from jax.experimental import pallas as pl
from jax.experimental.pallas import tpu as pltpu
from jax.sharding import PartitionSpec as P

NLON = 1536
KLON = 768
KLAT = 384
LEV = 3
ROWS = 48
COLS = 96
SUB = 3
PART = 16
CHUNKS = LEV * SUB
ACTIVE = 12
EARLY = 8
MESH = pl.DeviceIdType.MESH
F32 = jnp.float32
BF16 = jnp.bfloat16


def zonal_table():
    half = KLON // 2
    points = np.arange(NLON, dtype=np.int64)
    column = np.arange(KLON, dtype=np.int64)
    wave = np.where(column < half, column, column - half + 1)
    phase = points[:, None] * wave[None, :] % NLON
    angle = (np.float32(2.0 * np.pi / NLON) * phase.astype(np.float32)).astype(np.float32)
    scale = np.sqrt(np.float32(2.0 / NLON))
    values = np.where(column[None, :] < half, np.cos(angle), np.sin(angle)) * scale
    return values.astype(np.float32).astype(jnp.bfloat16)


def spread(tiles, lane):
    a, b, c = tiles
    rows = (
        a,
        pltpu.roll(jnp.where(lane >= 96, a, b), 32, 1),
        pltpu.roll(jnp.where(lane >= 64, b, c), 64, 1),
        pltpu.roll(c, 96, 1),
    )
    return [jnp.where(lane < COLS, r, 0.0) for r in rows]


def pack_rows(rows, lane):
    return [jnp.where(lane < COLS, rows[j], pltpu.roll(rows[3], 96 - 32 * j, 1)) for j in range(3)]


def unpack_rows(packed, lane):
    turned = [pltpu.roll(packed[j], 32 + 32 * j, 1) for j in range(3)]
    last = jnp.where(lane < 32, turned[0], jnp.where(lane < 64, turned[1], turned[2]))
    return [packed[0], packed[1], packed[2], last]


def rows_of_members(src, level, dst, base):
    for g in range(4):
        n = 8 if g < 3 else 7
        lane = lax.broadcasted_iota(jnp.int32, (n, 128), 1)
        for q in range(12):
            v = src[level, g * 8 : g * 8 + n, q * 384 : (q + 1) * 384].astype(F32)
            for r, row in enumerate(spread((v[:, :128], v[:, 128:256], v[:, 256:]), lane)):
                dst[pl.ds(base + g * 8 * ROWS + 4 * q + r, n, stride=ROWS), :] = row


def kernel(
    weight_hbm, control_hbm, perturbs_hbm, static_hbm, lat_hbm, local_hbm, stat_hbm, zonal_hbm,
    out_ref,
    weight_ref, static_ref, local_ref, stat_ref, control, perturbs, lat, zonal, tmp, tmps, pert,
    a_send, a_recv, c_send, c_recv, e_send, e_recv, g_send, g_recv, m_send, m_recv, rows_out, flat, turned, spc, spt, spec,
    in_sem, zon_sem, sa, ra, sc, rc, se, re, sg, rg, si, ri, sp,
):
    m = lax.axis_index("mem")
    z = lax.axis_index("lat")
    c = lax.axis_index("lon")
    quarter = lax.rem(z, 4)
    core = lax.rem(c, 2)

    def plan_of(level):
        return jnp.where(level == 1, 1, 0)

    def idle(level):
        return 3 - 2 * core - plan_of(level)

    def active(level):
        return quarter != idle(level)

    def block_of(device, level):
        part = lax.rem(device, 4)
        return 3 * (device // 4) + part - jnp.where(part > idle(level), 1, 0)


    def lon_peer(i):
        along, across = i // 4, 3 - lax.rem(i, 4)
        ahead = jnp.where(along == 3, 0, jnp.where(along == 2, 3, 2 - along))
        return 4 * lax.rem(c // 4 + ahead, 4) + lax.rem(lax.rem(c, 4) + across, 4)

    def far_first(i):
        step = (i + 1) // 2
        return 8 + jnp.where(lax.rem(i, 2) == 0, step, -step)

    loads = [
        pltpu.make_async_copy(control_hbm.at[k], control.at[k], in_sem.at[k]) for k in range(LEV)
    ]
    loads += [pltpu.make_async_copy(perturbs_hbm, perturbs, in_sem.at[3])]
    loads += [pltpu.make_async_copy(lat_hbm, lat, in_sem.at[4])]
    barrier = pltpu.get_barrier_semaphore()

    def greet(i, carry):
        pl.semaphore_signal(
            barrier, 1, device_id=(m, z, lax.rem(c + i, 16)), device_id_type=MESH
        )
        return carry

    def greet_far(i, carry):
        pl.semaphore_signal(
            barrier, 1, device_id=(m, lax.rem(z + far_first(i), 16), c), device_id_type=MESH
        )
        return carry

    lax.fori_loop(0, 15, greet_far, 0)
    lax.fori_loop(1, 16, greet, 0)
    pl.semaphore_signal(barrier, 1, device_id=(1 - m, z, c), device_id_type=MESH)

    small = [
        pltpu.make_async_copy(source, target, in_sem.at[5 + i])
        for i, (source, target) in enumerate(
            (
                (static_hbm, static_ref), (local_hbm, local_ref), (stat_hbm, stat_ref),
                (weight_hbm, weight_ref),
            )
        )
    ]
    for copy in loads[:1] + small + loads[1:]:
        copy.start()
    zonal_loads = [
        pltpu.make_async_copy(
            zonal_hbm.at[pl.ds(b * COLS, COLS)], zonal.at[b, pl.ds(0, COLS)], zon_sem.at[b]
        )
        for b in range(16)
    ]
    for copy in zonal_loads:
        copy.start()

    for copy in small:
        copy.wait()
    lane3 = lax.broadcasted_iota(jnp.int32, (LEV, 128), 1)
    for q in range(12):
        v = static_ref[:, q * 384 : (q + 1) * 384].astype(F32)
        for r, row in enumerate(spread((v[:, :128], v[:, 128:256], v[:, 256:]), lane3)):
            tmps[pl.ds(4 * q + r, LEV, stride=ROWS), :] = row

    lane8 = lax.broadcasted_iota(jnp.int32, (8, 128), 1)

    def split(block):
        return [block[8 * j : 8 * j + 8, :] for j in range(3)]

    def prepare(level):
        rows_of_members(control, level, tmp, 0)
        tmp[pl.ds(31 * ROWS, ROWS), :] = tmps[pl.ds(pl.multiple_of(level * ROWS, 8), ROWS), :]

        def pack(peer, carry):
            for s in range(SUB):
                rows = []
                for i in range(2):
                    for h in range(2):
                        start = pl.multiple_of((2 * peer + i) * ROWS + s * PART + 8 * h, 8)
                        rows.append(tmp[pl.ds(start, 8), :])
                a_send[level * SUB + s, peer] = jnp.concatenate(
                    pack_rows(rows, lane8), axis=0
                ).astype(BF16)
            return carry

        lax.fori_loop(0, 16, pack, 0)

    def send_rows(k):
        a_recv[k, c] = a_send[k, c]

        def step(i, carry):
            to = lon_peer(i)
            pltpu.make_async_remote_copy(
                a_send.at[k, to], a_recv.at[k, c], sa.at[k], ra.at[k],
                device_id=(m, z, to), device_id_type=MESH,
            ).start()
            return carry

        lax.fori_loop(0, 15, step, 0)

    loads[0].wait()
    prepare(0)
    spc[0] = local_ref[...]
    spc[1] = jnp.where(c == 15, stat_ref[...], local_ref[...])
    pl.semaphore_wait(barrier, 31)
    for k in range(SUB):
        send_rows(k)

    def share(plan, f, side, start, rows, at):
        send = 4 * plan + 2 * f + (1 if side > 0 else 0)
        return pltpu.make_async_remote_copy(
            spc.at[f, pl.ds(start, rows)], spt.at[plan, f, pl.ds(at, rows)],
            sp.at[send], sp.at[8 + 2 * plan + f],
            device_id=(m, lax.rem(z + 16 + side, 16), c), device_id_type=MESH,
        )

    pieces = []
    for plan in range(2):
        for which in range(2):
            users = [i for i in range(4) if i != 3 - 2 * which - plan]
            for block, user in enumerate(users):
                for owner in range(4):
                    low = max(64 * block, ROWS * owner)
                    high = min(64 * block + 64, ROWS * owner + ROWS)
                    if low < high:
                        start, at = low - ROWS * owner, low - 64 * block
                        pieces.append((plan, which, owner, user, start, high - low, at))

    def for_shared(todo, receiving):
        for plan, which, owner, user, start, rows, at in pieces:
            if owner == user:
                continue

            @pl.when((core == which) & (quarter == (user if receiving else owner)))
            def _():
                todo(share(plan, 0, user - owner, start, rows, at))

                @pl.when(c == 15)
                def _():
                    todo(share(plan, 1, user - owner, start, rows, at))

    for_shared(lambda copy: copy.start(), 0)

    for plan, which, owner, user, start, rows, at in pieces:
        if owner == user:

            @pl.when((core == which) & (quarter == owner))
            def _():
                spt[plan, :, at : at + rows, :] = spc[:, start : start + rows, :]

    for k in (1, 2):
        loads[k].wait()

    for b in range(16):
        zonal[b, COLS:, :] = jnp.zeros((128 - COLS, KLON), BF16)
    for copy in zonal_loads:
        copy.wait()

    lane16 = lax.broadcasted_iota(jnp.int32, (PART, 128), 1)

    def lay_out(level, carry):
        rows_of_members(perturbs, level, pert, level * (31 * ROWS))
        return carry

    def ready_to_filter():
        loads[3].wait()
        loads[4].wait()
        for_shared(lambda copy: copy.wait_recv(), 1)

        for plan in range(2):

            @pl.when(active(plan))
            def _():
                @pl.when(c < 15)
                def _():
                    spt[plan, 1] = spt[plan, 0]

                spec[plan] = spt[plan].reshape(128, KLAT).T

    def filter_of(level):
        merid = c_recv[level].reshape(16 * ROWS, 128)
        coef = lax.dot_general(
            lat[...], merid, (((0,), (0,)), ((), ())), preferred_element_type=F32
        )
        scaled = (coef * spec[plan_of(level)]).astype(BF16)
        for b in range(4):
            back = jnp.dot(
                lat[pl.ds(b * 4 * ROWS, 4 * ROWS), :], scaled, preferred_element_type=F32
            )
            e_send[level, pl.ds(4 * b, 4)] = back.astype(BF16).reshape(4, SUB, PART, 128)

    def spectral(level, carry):
        pltpu.make_async_copy(
            c_recv.at[level, pl.ds(0, 15)], c_recv.at[level, pl.ds(0, 15)], rc.at[level]
        ).wait()
        filter_of(level)
        own_block = block_of(z, level)

        for s in range(SUB):
            k = level * SUB + s
            e_recv[k, own_block] = e_send[level, z, s]

            def step(i, inner):
                to = lax.rem(z + far_first(i), 16)
                pltpu.make_async_remote_copy(
                    e_send.at[level, to, s], e_recv.at[k, own_block], se.at[k], re.at[k],
                    device_id=(m, to, c), device_id_type=MESH,
                ).start()
                return inner

            lax.fori_loop(0, 15, step, 0)
        return carry

    def waves_of(k):
        strips = jnp.concatenate(
            [
                jnp.concatenate(
                    unpack_rows(split(a_recv[k, b].astype(F32)), lane8), axis=0
                ).astype(BF16)
                for b in range(16)
            ],
            axis=1,
        )
        table = zonal[...].reshape(16 * 128, KLON)
        waves = jnp.dot(strips, table, preferred_element_type=F32)
        for t in range(6):
            first = waves[:PART, t * 128 : (t + 1) * 128]
            second = waves[PART:, t * 128 : (t + 1) * 128]
            c_send[k, 2 * t] = jnp.where(lane16 < 64, first, pltpu.roll(second, 64, 1)).astype(BF16)
            c_send[k, 2 * t + 1] = jnp.where(
                lane16 < 64, pltpu.roll(first, 64, 1), second
            ).astype(BF16)

    def to_waves(k, carry):
        pltpu.make_async_copy(
            a_recv.at[k, pl.ds(0, 15)], a_recv.at[k, pl.ds(0, 15)], ra.at[k]
        ).wait()
        waves_of(k)
        level, s = k // SUB, lax.rem(k, SUB)

        @pl.when(active(level))
        def _():
            c_recv[level, z, s] = c_send[k, block_of(z, level)]

        def step(i, inner):
            to = lax.rem(z + far_first(i), 16)

            @pl.when(lax.rem(to, 4) != idle(level))
            def _():
                pltpu.make_async_remote_copy(
                    c_send.at[k, block_of(to, level)], c_recv.at[level, z, s], sc.at[k],
                    rc.at[level], device_id=(m, to, c), device_id_type=MESH,
                ).start()

            return inner

        lax.fori_loop(0, 15, step, 0)

        @pl.when(k < CHUNKS - SUB)
        def _():
            @pl.when(s == 0)
            def _():
                prepare(level + 1)

            send_rows(k + SUB)

        @pl.when(k == CHUNKS - LEV - 2)
        def _():
            ready_to_filter()

        @pl.when((k >= CHUNKS - LEV - 1) & (k < CHUNKS - 1))
        def _():
            lay_out(k - (CHUNKS - LEV - 1), 0)

        @pl.when(active(0) & (k == EARLY))
        def _():
            spectral(0, 0)

        return carry

    lax.fori_loop(0, CHUNKS, to_waves, 0)

    def turn(b, carry):
        turned[:, pl.ds(pl.multiple_of(b * 128, 128), 128)] = zonal[b].T
        return carry

    lax.fori_loop(0, 16, turn, 0)

    for level in range(1, LEV):

        @pl.when(active(level))
        def _():
            spectral(level, 0)

    def grid_of(k):
        firsts, seconds = [], []
        for t in range(6):
            even = e_recv[k, 2 * t].astype(F32)
            odd = e_recv[k, 2 * t + 1].astype(F32)
            firsts.append(jnp.where(lane16 < 64, even, pltpu.roll(odd, 64, 1)))
            seconds.append(jnp.where(lane16 < 64, pltpu.roll(even, 64, 1), odd))
        rows = jnp.concatenate(
            [jnp.concatenate(firsts, axis=1), jnp.concatenate(seconds, axis=1)], axis=0
        ).astype(BF16)
        for b in range(4):
            grid = lax.dot_general(
                rows, turned[:, b * 512 : (b + 1) * 512], (((1,), (0,)), ((), ())),
                preferred_element_type=F32,
            )
            for i in range(4):
                tiles = [
                    grid[8 * j : 8 * j + 8, i * 128 : (i + 1) * 128] for j in range(4)
                ]
                g_send[k, 4 * b + i] = jnp.concatenate(
                    pack_rows(tiles, lane8), axis=0
                ).astype(BF16)

    def to_grid(k, carry):
        for here, count in ((True, ACTIVE - 1), (False, ACTIVE)):

            @pl.when(active(k // SUB) == here)
            def _():
                pltpu.make_async_copy(
                    e_recv.at[k, pl.ds(0, count)], e_recv.at[k, pl.ds(0, count)], re.at[k]
                ).wait()

        grid_of(k)
        g_recv[k, c] = g_send[k, c]

        def step(i, inner):
            to = lon_peer(i)
            pltpu.make_async_remote_copy(
                g_send.at[k, to], g_recv.at[k, c], sg.at[k], rg.at[k],
                device_id=(m, z, to), device_id_type=MESH,
            ).start()
            return inner

        lax.fori_loop(0, 15, step, 0)
        return carry

    lax.fori_loop(0, CHUNKS, to_grid, 0)

    first_mem = jnp.where(m == 0, 1.0, 0.0).astype(F32)

    def across(k):
        return pltpu.make_async_remote_copy(
            m_send.at[k], m_recv.at[k], si.at[k], ri.at[k],
            device_id=(1 - m, z, c), device_id_type=MESH,
        )

    def product_of(k, level, s):
        total = [jnp.zeros((8, 128), F32), jnp.zeros((8, 128), F32)]
        for peer in range(16):
            rows = unpack_rows(split(g_recv[k, peer].astype(F32)), lane8)
            for i in range(2 if peer < 15 else 1):
                for h in range(2):
                    start = level * (31 * ROWS) + (2 * peer + i) * ROWS + s * PART + 8 * h
                    total[h] += pert[pl.ds(pl.multiple_of(start, 8), 8), :] * rows[2 * i + h]
        weight = weight_ref[level]
        parts = [
            first_mem * weight * rows[2 + h] + (1.0 - weight) * total[h] for h in range(2)
        ]
        return jnp.concatenate(parts, axis=0)

    def product(k, carry):
        pltpu.make_async_copy(
            g_recv.at[k, pl.ds(0, 15)], g_recv.at[k, pl.ds(0, 15)], rg.at[k]
        ).wait()
        level, s = k // SUB, lax.rem(k, SUB)
        m_send[k] = product_of(k, level, s)
        across(k).start()
        return carry

    lax.fori_loop(0, CHUNKS, product, 0)

    for_shared(lambda copy: copy.wait_send(), 0)

    def drain(k, carry):
        for ref, sem in ((a_send, sa), (g_send, sg)):
            pltpu.make_async_copy(
                ref.at[k, pl.ds(0, 15)], ref.at[k, pl.ds(0, 15)], sem.at[k]
            ).wait()
        for here, count in ((True, ACTIVE - 1), (False, ACTIVE)):

            @pl.when(active(k // SUB) == here)
            def _():
                pltpu.make_async_copy(
                    c_send.at[k, pl.ds(0, count)], c_send.at[k, pl.ds(0, count)], sc.at[k]
                ).wait()

        @pl.when(active(k // SUB))
        def _():
            pltpu.make_async_copy(
                e_send.at[k // SUB, pl.ds(0, 15), 0], e_send.at[k // SUB, pl.ds(0, 15), 0], se.at[k]
            ).wait()

        return carry

    lax.fori_loop(0, CHUNKS, drain, 0)

    def finish(k, carry):
        across(k).wait()
        rows_out[pl.ds(pl.multiple_of(k * PART, 8), PART), :] = m_send[k] + m_recv[k]
        return carry

    lax.fori_loop(0, CHUNKS, finish, 0)
    quads = LEV * ROWS // 4
    lane36 = lax.broadcasted_iota(jnp.int32, (quads, 128), 1)
    first, second, third, fourth = (rows_out[pl.ds(r, quads, stride=4), :] for r in range(4))
    second, third = pltpu.roll(second, 96, 1), pltpu.roll(third, 64, 1)
    fourth = pltpu.roll(fourth, 32, 1)
    flat[pl.ds(0, quads, stride=3), :] = jnp.where(lane36 < 96, first, second)
    flat[pl.ds(1, quads, stride=3), :] = jnp.where(lane36 < 64, second, third)
    flat[pl.ds(2, quads, stride=3), :] = jnp.where(lane36 < 32, third, fourth)

    out_ref[...] = flat[...].reshape(out_ref.shape)


def shards(
    control, perturbs, static_input, lat_basis, local_spectrum, static_spectrum, static_weight
):
    by_level = lambda a: jnp.swapaxes(a.reshape(31, LEV, ROWS * COLS), 0, 1)
    vmem = pl.BlockSpec(memory_space=pltpu.VMEM)
    hbm = pl.BlockSpec(memory_space=pltpu.HBM)
    dma = pltpu.SemaphoreType.DMA
    out = pl.pallas_call(
        kernel,
        out_shape=jax.ShapeDtypeStruct((LEV * ROWS * COLS // 128, 1, 128), F32),
        in_specs=[
            hbm, hbm, hbm, hbm, hbm, hbm, hbm, hbm,
        ],
        out_specs=vmem,
        scratch_shapes=[
            pltpu.SMEM((LEV,), F32),
            pltpu.VMEM((LEV, ROWS * COLS), BF16),
            pltpu.VMEM((ROWS, KLAT), F32),
            pltpu.VMEM((ROWS, KLAT), F32),
            pltpu.VMEM((LEV, 31, ROWS * COLS), BF16),
            pltpu.VMEM((LEV, 31, ROWS * COLS), BF16),
            pltpu.VMEM((16 * ROWS, KLAT), BF16),
            pltpu.VMEM((16, 128, KLON), BF16),
            pltpu.VMEM((32 * ROWS, 128), F32),
            pltpu.VMEM((LEV * ROWS, 128), F32),
            pltpu.VMEM((LEV * 31 * ROWS, 128), F32),
            pltpu.VMEM((CHUNKS, 16, 24, 128), BF16),
            pltpu.VMEM((CHUNKS, 16, 24, 128), BF16),
            pltpu.VMEM((CHUNKS, ACTIVE, PART, 128), BF16),
            pltpu.VMEM((LEV, 16, SUB, PART, 128), BF16),
            pltpu.VMEM((LEV, 16, SUB, PART, 128), BF16),
            pltpu.VMEM((CHUNKS, ACTIVE, PART, 128), BF16),
            pltpu.VMEM((CHUNKS, 16, 24, 128), BF16),
            pltpu.VMEM((CHUNKS, 16, 24, 128), BF16),
            pltpu.VMEM((CHUNKS, PART, 128), F32),
            pltpu.VMEM((CHUNKS, PART, 128), F32),
            pltpu.VMEM((LEV * ROWS, 128), F32),
            pltpu.VMEM((LEV * ROWS * COLS // 128, 128), F32),
            pltpu.VMEM((KLON, 16 * 128), BF16),
            pltpu.VMEM((2, ROWS, KLAT), F32),
            pltpu.VMEM((2, 2, 64, KLAT), F32),
            pltpu.VMEM((2, KLAT, 128), F32),
            dma((9,)),
            dma((16,)),
        ]
        + [dma((CHUNKS,))] * 3
        + [dma((LEV,))]
        + [dma((CHUNKS,))] * 6
        + [dma((12,))],
        compiler_params=pltpu.CompilerParams(
            collective_id=0, has_side_effects=True, vmem_limit_bytes=60 * 1024 * 1024
        ),
    )(
        static_weight,
        by_level(control),
        by_level(perturbs),
        static_input.reshape(LEV, ROWS * COLS),
        lat_basis,
        local_spectrum.T,
        static_spectrum.T,
        jnp.asarray(zonal_table()),
    )
    return out.reshape(LEV, 1, 1, ROWS * COLS)


def solution(mesh):
    in_specs = (
        P("mem", None, "lat", "lon", None),
        P("mem", None, "lat", "lon", None),
        P(None, "lat", "lon", None),
        P(),
        P(None, "lat"),
        P(None, "lat"),
        P(),
    )
    return jax.shard_map(
        shards, mesh=mesh, in_specs=in_specs, out_specs=P(None, "lat", "lon", None), check_vma=False
    )
```
